8 devices in a mesh: dp: 1 (over z), ctx: 8 (over y, x, core).
Axes of the slice: x: 2, y: 2, z: 1, core: 2. Of those that a mesh axis runs over, the one named last changes fastest.
Arguments:
- hidden: bfloat16 [256, 2048], P(('dp', 'ctx'))
- w_q: bfloat16 [2048, 3072], replicated
- w_uk: bfloat16 [16, 128, 512], replicated
- w_uv: bfloat16 [16, 512, 128], replicated
- w_o: bfloat16 [2048, 2048], replicated
- kv_prefix: bfloat16 [16384, 576], P(('dp', 'ctx'))
- kv_suffix: bfloat16 [256, 2048, 576], P(('dp', 'ctx'))
- seq_lens: int32 [256], P(('dp', 'ctx'))
Outputs:
- output: bfloat16 [256, 2048], P(('dp', 'ctx'))
All inputs are finite; a program needn't handle non-finite values.
Results may differ from the reference program's by a relative error of at most 0.00657996.
Values are sent between devices in bfloat16 or wider.
A program may use at most 1 GiB of HBM per device.

```python
import math
import jax
import jax.numpy as jnp
from jax import lax

MODEL_DIM = 2048
HEADS = 16
NOPE_DIM = 128
ROPE_DIM = 64
VALUE_DIM = 128
LATENT_DIM = 512
GROUP_SIZE = 8
SEQUENCES = 256
PREFIX_LEN = 16384
SUFFIX_LEN = 2048
ROPE_BASE = 10000

KV_WIDTH = LATENT_DIM + ROPE_DIM
QK_WIDTH = NOPE_DIM + ROPE_DIM
SCORE_SCALE = QK_WIDTH ** -0.5
BLOCK_LEN = PREFIX_LEN // GROUP_SIZE
PREFIX_AMP = 1.5
SUFFIX_AMP = PREFIX_AMP * math.sqrt(1.0 + 2.0 * math.log(max(2.0 * PREFIX_LEN / SUFFIX_LEN, 1.0)) * QK_WIDTH / (PREFIX_AMP ** 2 * LATENT_DIM))


def draw_lengths(key):
    raw_lens = jax.random.randint(key, (SEQUENCES,), 0, SUFFIX_LEN, jnp.int32)
    seq_index = jnp.arange(SEQUENCES)
    return jnp.where(seq_index == 0, SUFFIX_LEN - 1, jnp.where(seq_index == 1, 0, raw_lens)).astype(jnp.int32)


def latent_cache(noise, means):
    rope_pad = jnp.zeros(means.shape[:-1] + (ROPE_DIM,), jnp.float32)
    return noise + jnp.concatenate([means, rope_pad], axis=-1)


def setup_inputs(seed: int = 0, part: int = 0) -> dict:
    shared_keys = jax.random.split(jax.random.key(seed + 1), 4)
    own_keys = jax.random.split(jax.random.fold_in(jax.random.key(seed), part), 6)
    hidden = jax.random.normal(own_keys[0], (SEQUENCES, MODEL_DIM), jnp.float32)
    w_q = jax.random.normal(shared_keys[0], (MODEL_DIM, HEADS * QK_WIDTH), jnp.float32) * MODEL_DIM ** -0.5
    w_uk = jax.random.normal(shared_keys[1], (HEADS, NOPE_DIM, LATENT_DIM), jnp.float32) * NOPE_DIM ** -0.5
    w_uv = jax.random.normal(shared_keys[2], (HEADS, LATENT_DIM, VALUE_DIM), jnp.float32) * LATENT_DIM ** -0.5
    w_o = jax.random.normal(shared_keys[3], (HEADS * VALUE_DIM, MODEL_DIM), jnp.float32) * (HEADS * VALUE_DIM) ** -0.5
    pre_noise = jax.random.normal(own_keys[1], (GROUP_SIZE, BLOCK_LEN, KV_WIDTH), jnp.float32)
    pre_means = jax.random.normal(own_keys[2], (GROUP_SIZE, 1, LATENT_DIM), jnp.float32) * PREFIX_AMP
    kv_prefix = latent_cache(pre_noise, pre_means).reshape(PREFIX_LEN, KV_WIDTH)
    suf_noise = jax.random.normal(own_keys[3], (SEQUENCES, SUFFIX_LEN, KV_WIDTH), jnp.float32)
    suf_means = jax.random.normal(own_keys[4], (SEQUENCES, 1, LATENT_DIM), jnp.float32) * SUFFIX_AMP
    kv_suffix = latent_cache(suf_noise, suf_means)
    seq_lens = draw_lengths(own_keys[5])
    return {'hidden': hidden.astype(jnp.bfloat16), 'w_q': w_q.astype(jnp.bfloat16), 'w_uk': w_uk.astype(jnp.bfloat16), 'w_uv': w_uv.astype(jnp.bfloat16), 'w_o': w_o.astype(jnp.bfloat16), 'kv_prefix': kv_prefix.astype(jnp.bfloat16), 'kv_suffix': kv_suffix.astype(jnp.bfloat16), 'seq_lens': seq_lens}


def rope_rotate(rot_in, positions):
    half_dim = ROPE_DIM // 2
    inv_freq = jnp.exp(jnp.arange(half_dim, dtype=jnp.float32) * (-math.log(ROPE_BASE) / half_dim))
    angle = positions.astype(jnp.float32)[:, None, None] * inv_freq
    cos_part = jnp.cos(angle)
    sin_part = jnp.sin(angle)
    rot_wide = rot_in.astype(jnp.float32)
    first_half = rot_wide[..., :half_dim]
    second_half = rot_wide[..., half_dim:]
    return jnp.concatenate([first_half * cos_part - second_half * sin_part, second_half * cos_part + first_half * sin_part], axis=-1)


def reference(hidden, w_q, w_uk, w_uv, w_o, kv_prefix, kv_suffix, seq_lens):
    q_all = jnp.dot(hidden, w_q, preferred_element_type=jnp.float32).astype(jnp.bfloat16).reshape(SEQUENCES, HEADS, QK_WIDTH)
    q_lat = jnp.einsum('bhn,hnc->bhc', q_all[..., :NOPE_DIM].astype(jnp.float32), w_uk.astype(jnp.float32)).astype(jnp.bfloat16)
    q_rot = rope_rotate(q_all[..., NOPE_DIM:], PREFIX_LEN + seq_lens).astype(jnp.bfloat16)
    query = jnp.concatenate([q_lat, q_rot], axis=-1)
    pre_keys = kv_prefix.astype(jnp.float32)
    pre_vals = pre_keys[:, :LATENT_DIM]
    slots = jnp.arange(SUFFIX_LEN)

    def one_sequence(item):
        q_row, suf_row, length = item
        q_row = q_row.astype(jnp.float32)
        suf_keys = suf_row.astype(jnp.float32)
        s_pre = jnp.einsum('hw,pw->hp', q_row, pre_keys) * SCORE_SCALE
        s_suf = jnp.einsum('hw,sw->hs', q_row, suf_keys) * SCORE_SCALE
        s_suf = jnp.where((slots <= length)[None, :], s_suf, -jnp.inf)
        probs = jax.nn.softmax(jnp.concatenate([s_pre, s_suf], axis=-1), axis=-1)
        return jnp.dot(probs[:, :PREFIX_LEN], pre_vals) + jnp.dot(probs[:, PREFIX_LEN:], suf_keys[:, :LATENT_DIM])

    o_lat = lax.map(one_sequence, (query, kv_suffix, seq_lens)).astype(jnp.bfloat16)
    o_val = jnp.einsum('bhc,hcv->bhv', o_lat.astype(jnp.float32), w_uv.astype(jnp.float32)).astype(jnp.bfloat16)
    out = hidden.astype(jnp.float32) + jnp.dot(o_val.reshape(SEQUENCES, HEADS * VALUE_DIM), w_o, preferred_element_type=jnp.float32)
    return out.astype(jnp.bfloat16)
```

```python
import functools
import math
import jax
import jax.numpy as jnp
from jax import lax
from jax.experimental import pallas as pl
from jax.experimental.pallas import tpu as pltpu
from jax.sharding import PartitionSpec as P

ROPE_BASE = 10000
LOG2E = 1.4426950408889634
NT = (((1,), (1,)), ((), ()))
F32 = jnp.float32
BF16 = jnp.bfloat16
MIB = 1024 * 1024
TAIL = 8


def vmem():
    return pl.BlockSpec(memory_space=pltpu.VMEM)


def hbm():
    return pl.BlockSpec(memory_space=pl.ANY)


def query_kernel(n_head, nope, rope, hid_ref, trig_ref, rot_ref, wq_hbm, wuk_hbm, kv_hbm,
                 q_ref, qs_ref, kvs_hbm,
                 hid_all, trig_all, wq_v, wuk_v, qs_f, wq_sem, wuk_sem, send_sem, recv_sem):
    rows = hid_ref.shape[0]
    lat = wuk_v.shape[2]
    qk = nope + rope
    per = 4
    groups = n_head // per
    width = per * qk
    me = lax.axis_index('ctx')
    core = lax.rem(me, 2)
    xx = lax.rem(me // 2, 2)
    yy = me // 4
    sib = me + 1 - 2 * core
    to_x = me + 2 - 4 * xx
    to_y = me + 4 - 8 * yy
    to_d = me + 6 - 4 * xx - 8 * yy
    weights = []
    for g in range(groups):
        cols = pl.ds(g * width, width)
        copy = pltpu.make_async_copy(wq_hbm.at[:, cols], wq_v.at[:, cols], wq_sem.at[g])
        copy.start()
        weights.append(copy)
    wuk_copy = pltpu.make_async_copy(wuk_hbm, wuk_v, wuk_sem)
    wuk_copy.start()

    barrier = pltpu.get_barrier_semaphore()
    for peer in (sib, to_x, to_y, to_d):
        pl.semaphore_signal(barrier, inc=1, device_id={'ctx': peer})
    pl.semaphore_wait(barrier, 4)
    sends = []
    for slot, peer in ((2, to_d), (0, to_x), (1, to_y)):
        sends.append(pltpu.make_async_remote_copy(
            src_ref=hid_ref, dst_ref=hid_all.at[slot], send_sem=send_sem.at[slot], recv_sem=recv_sem.at[slot],
            device_id={'ctx': peer}))
        sends.append(pltpu.make_async_remote_copy(
            src_ref=trig_ref, dst_ref=trig_all.at[slot], send_sem=send_sem.at[3 + slot], recv_sem=recv_sem.at[3 + slot],
            device_id={'ctx': peer}))
    sends.append(pltpu.make_async_remote_copy(
        src_ref=kv_hbm, dst_ref=kvs_hbm, send_sem=send_sem.at[6], recv_sem=recv_sem.at[6], device_id={'ctx': sib}))
    for copy in sends:
        copy.start()

    def project(hid, cos, sin, g, store):
        q_all = jnp.dot(hid, wq_v[:, g * width:(g + 1) * width], preferred_element_type=F32)
        for j in range(per):
            h = g * per + j
            q_nope = q_all[:, j * qk:j * qk + nope].astype(BF16)
            q_pe = q_all[:, j * qk + nope:(j + 1) * qk].astype(BF16)
            q_lat = jnp.dot(q_nope, wuk_v[h], preferred_element_type=F32).astype(BF16)
            turned = jnp.dot(q_pe, rot_ref[...], preferred_element_type=F32)
            q_rot = (q_pe.astype(F32) * cos + turned * sin).astype(BF16)
            store(h, q_lat, q_rot)

    def store_own(h, q_lat, q_rot):
        q_ref[3, h, :, 0:lat] = q_lat
        q_ref[3, h, :, lat:lat + rope] = q_rot
        for n in range(lat // 128):
            qs_f[n, pl.ds(h, rows, stride=n_head), :] = q_lat[:, n * 128:(n + 1) * 128].astype(F32)
        wide_rot = jnp.concatenate([q_rot, q_rot], axis=1).astype(F32)
        qs_f[lat // 128, pl.ds(h, rows, stride=n_head), :] = wide_rot

    def store_peer(h, q_lat, q_rot):
        for p in range(3):
            q_ref[p, h, :, 0:lat] = q_lat[p * rows:(p + 1) * rows]
            q_ref[p, h, :, lat:lat + rope] = q_rot[p * rows:(p + 1) * rows]

    wuk_copy.wait()
    for g in range(groups):
        weights[g].wait()
        project(hid_ref[...], trig_ref[0], trig_ref[1], g, store_own)
    for n in range(lat // 128):
        qs_ref[:, n * 128:(n + 1) * 128] = qs_f[n].astype(BF16)
    qs_ref[:, lat:lat + rope] = qs_f[lat // 128][:, 0:rope].astype(BF16)
    for copy in sends[:-1]:
        copy.wait()
    hid3 = hid_all[...].reshape(3 * rows, hid_ref.shape[1])
    cos3 = jnp.concatenate([trig_all[p, 0] for p in range(3)], axis=0)
    sin3 = jnp.concatenate([trig_all[p, 1] for p in range(3)], axis=0)
    for g in range(groups):
        project(hid3, cos3, sin3, g, store_peer)
    sends[-1].wait()


def make_queries(hidden, w_q, w_uk, kv_own, seq_lens, first_pos):
    rows, dim = hidden.shape
    n_head, nope, lat = w_uk.shape
    qk = w_q.shape[1] // n_head
    rope = qk - nope
    half = rope // 2
    inv_freq = jnp.exp(jnp.arange(half, dtype=F32) * (-math.log(ROPE_BASE) / half))
    angle = (first_pos + seq_lens).astype(F32)[:, None] * inv_freq
    cos_part, sin_part = jnp.cos(angle), jnp.sin(angle)
    trig = jnp.stack([jnp.concatenate([cos_part, cos_part], -1), jnp.concatenate([sin_part, sin_part], -1)])
    i, j = jnp.arange(rope)[:, None], jnp.arange(rope)[None, :]
    rot = jnp.where(i == j + half, -1.0, jnp.where(i + half == j, 1.0, 0.0)).astype(BF16)
    return pl.pallas_call(
        functools.partial(query_kernel, n_head, nope, rope),
        out_shape=(jax.ShapeDtypeStruct((4, n_head, rows, lat + rope), BF16),
                   jax.ShapeDtypeStruct((rows * n_head, lat + rope), BF16),
                   jax.ShapeDtypeStruct(kv_own.shape, BF16)),
        in_specs=[vmem(), vmem(), vmem(), hbm(), hbm(), hbm()],
        out_specs=(vmem(), vmem(), hbm()),
        scratch_shapes=[
            pltpu.VMEM((3, rows, dim), BF16), pltpu.VMEM((3, 2, rows, rope), F32),
            pltpu.VMEM(w_q.shape, BF16), pltpu.VMEM(w_uk.shape, BF16),
            pltpu.VMEM((lat // 128 + 1, rows * n_head, 128), F32),
            pltpu.SemaphoreType.DMA((n_head // 4,)), pltpu.SemaphoreType.DMA,
            pltpu.SemaphoreType.DMA((7,)), pltpu.SemaphoreType.DMA((7,))],
        compiler_params=pltpu.CompilerParams(collective_id=0, has_side_effects=True, vmem_limit_bytes=40 * MIB),
        name='queries',
    )(hidden, trig, rot, w_q, w_uk, kv_own)


def softmax_step(s, m_ref, l_ref, log2_scale):
    m_old = m_ref[:, 0:1]
    m_new = jnp.maximum(m_old, jnp.max(s, axis=1, keepdims=True))
    alpha = jnp.exp2((m_old - m_new) * log2_scale)
    p = jnp.exp2((s - m_new) * log2_scale)
    l_new = l_ref[:, 0:1] * alpha + jnp.sum(p, axis=1, keepdims=True)
    m_ref[...] = jnp.broadcast_to(m_new, m_ref.shape)
    l_ref[...] = jnp.broadcast_to(l_new, l_ref.shape)
    return p.astype(BF16), alpha


def prefix_kernel(log2_scale, lat, carried, *refs):
    if carried:
        qa_ref, qb_ref, ka_ref, kb_ref, ca_ref, cb_ref, oa_ref, ob_ref, q_v, m_v, l_v, acc = refs
    else:
        qa_ref, qb_ref, ka_ref, kb_ref, oa_ref, ob_ref, q_v, m_v, l_v, acc = refs
    half = qa_ref.shape[1]
    step = pl.program_id(0)

    @pl.when(step == 0)
    def _():
        q_v[0:half] = qa_ref[0]
        q_v[half:] = qb_ref[0]
        if carried:
            for n, c_ref in enumerate((ca_ref, cb_ref)):
                at = slice(n * half, (n + 1) * half)
                acc[at] = c_ref[0:half]
                m_col = jnp.transpose(c_ref[half:half + TAIL, 0:half])[:, 0:1]
                l_col = jnp.transpose(c_ref[half:half + TAIL, half:2 * half])[:, 0:1]
                m_v[at] = jnp.broadcast_to(m_col, (half, 128))
                l_v[at] = jnp.broadcast_to(l_col, (half, 128))
        else:
            acc[...] = jnp.zeros_like(acc)
            m_v[...] = jnp.full_like(m_v, -jnp.inf)
            l_v[...] = jnp.zeros_like(l_v)

    q = q_v[...]
    s_a = jnp.dot(q, ka_ref[...], preferred_element_type=F32)
    s_b = jnp.dot(q, kb_ref[...], preferred_element_type=F32)
    p_a, alpha_a = softmax_step(s_a, m_v, l_v, log2_scale)
    acc[...] = acc[...] * alpha_a + lax.dot_general(p_a, ka_ref[0:lat, :], NT, preferred_element_type=F32)
    p_b, alpha_b = softmax_step(s_b, m_v, l_v, log2_scale)
    acc[...] = acc[...] * alpha_b + lax.dot_general(p_b, kb_ref[0:lat, :], NT, preferred_element_type=F32)

    @pl.when(step == pl.num_programs(0) - 1)
    def _():
        for n, o_ref in enumerate((oa_ref, ob_ref)):
            at = slice(n * half, (n + 1) * half)
            o_ref[0:half] = acc[at]
            o_ref[half:half + TAIL, 0:half] = jnp.transpose(m_v[at])[0:TAIL]
            o_ref[half:half + TAIL, half:2 * half] = jnp.transpose(l_v[at])[0:TAIL]


def prefix_part(q_blocks, kv_own, kv_sib, pick_a, pick_b, log2_scale, lat, carry=None, block=512):
    half, wide = q_blocks.shape[1:]
    steps = kv_own.shape[1] // block
    payload = jax.ShapeDtypeStruct((half + TAIL, lat), F32)
    whole = pl.BlockSpec((half + TAIL, lat), lambda i: (0, 0))
    keys = pl.BlockSpec((wide, block), lambda i: (0, i))
    carry = () if carry is None else tuple(carry)
    flops = 2 * 2 * half * 2 * kv_own.shape[1] * (wide + lat)
    return pl.pallas_call(
        functools.partial(prefix_kernel, log2_scale, lat, bool(carry)),
        grid=(steps,),
        out_shape=(payload, payload),
        in_specs=[pl.BlockSpec((1, half, wide), lambda i: (pick_a, 0, 0)),
                  pl.BlockSpec((1, half, wide), lambda i: (pick_b, 0, 0)), keys, keys] + [whole] * len(carry),
        out_specs=(whole, whole),
        scratch_shapes=[pltpu.VMEM((2 * half, wide), BF16), pltpu.VMEM((2 * half, 128), F32),
                        pltpu.VMEM((2 * half, 128), F32), pltpu.VMEM((2 * half, lat), F32)],
        compiler_params=pltpu.CompilerParams(vmem_limit_bytes=32 * MIB),
        cost_estimate=pl.CostEstimate(flops=flops, bytes_accessed=8 * MIB, transcendentals=0),
        name='prefix',
    )(q_blocks, q_blocks, kv_own, kv_sib, *carry)


def suffix_kernel(log2_scale, lat, chunk, unit, n_buf, lens_ref, q_ref, kv_hbm, o_ref, m_ref, l_ref,
                  kv_v, s_v, p_v, a_v, m_v, l_v, acc, sems):
    n_seq = lens_ref.shape[0]
    heads = q_ref.shape[0] // n_seq
    total = jnp.int32(0)
    for b in range(n_seq):
        total += lens_ref[b] // chunk + 1
    trips = lax.div(total + unit - 1, unit)
    depth = n_buf // unit - 3

    def length(b):
        return lens_ref[jnp.minimum(b, n_seq - 1)]

    def fetch(b, c, slot):
        return pltpu.make_async_copy(
            kv_hbm.at[b, :, pl.ds(pl.multiple_of(c * chunk, chunk), chunk)], kv_v.at[slot], sems.at[slot])

    def advance(b, c):
        last = c >= length(b) // chunk
        return jnp.where(last, jnp.minimum(b + 1, n_seq), b), jnp.where(last, 0, c + 1)

    def prime(j, at):
        b, c = at

        @pl.when(b < n_seq)
        def _():
            fetch(b, c, j).start()
        return advance(b, c)

    zero, none = jnp.int32(0), jnp.int32(n_seq)
    ahead = lax.fori_loop(0, depth * unit, prime, (zero, zero))

    def step(i, at):
        fetched, scored, softened = at[0:2], at[2:2 + 2 * unit], at[2 + 2 * unit:]
        base = lax.rem(i, n_buf // unit) * unit
        far = lax.rem(i + depth, n_buf // unit) * unit
        back = lax.rem(i + n_buf // unit - 2, n_buf // unit) * unit
        items = []
        if True:
            b, c = fetched
            for u in range(unit):
                @pl.when(b < n_seq)
                def _(b=b, c=c, u=u):
                    fetch(b, c, far + u).start()
                b, c = advance(b, c)
            fetched = (b, c)
        b, c = at[-2:]
        for u in range(unit):
            @pl.when(b < n_seq)
            def _(b=b, c=c, u=u):
                fetch(b, c, base + u).wait()
            items += [b, c]
            b, c = advance(b, c)
        head = (b, c)

        acc_old = acc[unit - 1]
        for u in range(unit):
            pv = lax.dot_general(kv_v[back + u, 0:lat, :], p_v[u], NT, preferred_element_type=F32)
            first = softened[2 * u + 1] == 0
            acc_old = jnp.where(first, 0.0, acc_old * a_v[u, 0:1, 0:heads]) + pv
            acc[u] = acc_old

        m_old, l_old = m_v[:, 0:1], l_v[:, 0:1]
        for u in range(unit):
            b, c = scored[2 * u], scored[2 * u + 1]
            first = c == 0
            pos = c * chunk + lax.broadcasted_iota(jnp.int32, (heads, chunk), 1)
            s = jnp.where(pos <= length(b), s_v[u], -jnp.inf)
            m_old = jnp.where(first, -jnp.inf, m_old)
            m_new = jnp.maximum(m_old, jnp.max(s, axis=1, keepdims=True))
            alpha = jnp.exp2((m_old - m_new) * log2_scale)
            p = jnp.exp2((s - m_new) * log2_scale)
            l_old = jnp.where(first, 0.0, l_old) * alpha + jnp.sum(p, axis=1, keepdims=True)
            m_old = m_new
            p_v[u] = p.astype(BF16)
            a_v[u] = jnp.transpose(jnp.broadcast_to(alpha, (heads, 128)))[0:8]
            out = pl.ds(pl.multiple_of(b * heads, heads), heads)
            m_full, l_full = jnp.broadcast_to(m_old, m_v.shape), jnp.broadcast_to(l_old, l_v.shape)
            m_ref[out, :] = m_full
            l_ref[out, :] = l_full
        m_v[...] = m_full
        l_v[...] = l_full

        for u in range(unit):
            bq = jnp.minimum(items[2 * u], n_seq - 1)
            q = q_ref[pl.ds(pl.multiple_of(bq * heads, heads), heads), :]
            s_v[u] = jnp.dot(q, kv_v[base + u], preferred_element_type=F32)

        for u in range(unit):
            b, c = softened[2 * u], softened[2 * u + 1]

            @pl.when(jnp.logical_and(b < n_seq, c >= length(b) // chunk))
            def _(b=b, u=u):
                out = pl.ds(pl.multiple_of(b * heads, heads), heads)
                whole = jnp.transpose(acc[u])
                for n in range(lat // 128):
                    o_ref[n, out, :] = whole[:, n * 128:(n + 1) * 128]
        return (*fetched, *items, *scored, *head)

    lax.fori_loop(0, trips + 2, step, (*ahead, *(none, zero) * (2 * unit), zero, zero))


def suffix_part(q_seq, kv_suffix, seq_lens, log2_scale, lat, chunk=512, unit=2, n_buf=16):
    n_seq, slots, wide = kv_suffix.shape
    rows = q_seq.shape[0]
    heads = rows // n_seq
    flops = 2 * rows * slots * (wide + lat) * 4
    return pl.pallas_call(
        functools.partial(suffix_kernel, log2_scale, lat, chunk, unit, n_buf),
        out_shape=(jax.ShapeDtypeStruct((lat // 128, rows, 128), F32), jax.ShapeDtypeStruct((rows + heads, 128), F32),
                   jax.ShapeDtypeStruct((rows + heads, 128), F32)),
        in_specs=[pl.BlockSpec(memory_space=pltpu.SMEM), vmem(), hbm()],
        out_specs=(vmem(), vmem(), vmem()),
        scratch_shapes=[pltpu.VMEM((n_buf, wide, chunk), BF16), pltpu.VMEM((unit, heads, chunk), F32),
                        pltpu.VMEM((unit, heads, chunk), BF16), pltpu.VMEM((unit, 8, heads), F32),
                        pltpu.VMEM((heads, 128), F32), pltpu.VMEM((heads, 128), F32),
                        pltpu.VMEM((unit, lat, heads), F32), pltpu.SemaphoreType.DMA((n_buf,))],
        compiler_params=pltpu.CompilerParams(vmem_limit_bytes=24 * MIB),
        cost_estimate=pl.CostEstimate(flops=flops, bytes_accessed=40 * MIB, transcendentals=0),
        name='suffix',
    )(seq_lens, q_seq, kv_suffix.swapaxes(1, 2))


def output_kernel(log2_scale, hid_ref, wuv_ref, wo_ref, so_ref, sm_ref, sl_ref, *refs):
    parts, out_ref, v_v = refs[:6], refs[6], refs[7]
    n_head = wuv_ref.shape[0]
    rows = hid_ref.shape[0]
    half = n_head // 2
    block = half * rows
    value = wuv_ref.shape[2]
    cols = []
    for part in parts:
        m_t = jnp.transpose(part[block:block + TAIL, 0:block])
        l_t = jnp.transpose(part[block:block + TAIL, block:2 * block])
        cols.append((m_t[:, 0:1], l_t[:, 0:1]))
    for h in range(n_head):
        side, at = h // half, (h % half) * rows
        mine = pl.ds(h, rows, stride=n_head)
        own = jnp.concatenate([so_ref[n, mine, :] for n in range(so_ref.shape[0])], axis=1)
        terms = [(own, sm_ref[mine, :][:, 0:1], sl_ref[mine, :][:, 0:1])]
        for n in range(side, 6, 2):
            terms.append((parts[n][at:at + rows, :], cols[n][0][at:at + rows], cols[n][1][at:at + rows]))
        m_all = functools.reduce(jnp.maximum, [t[1] for t in terms])
        o_sum, l_sum = 0.0, 0.0
        for o_part, m_part, l_part in terms:
            weight = jnp.exp2((m_part - m_all) * log2_scale)
            o_sum += o_part * weight
            l_sum += l_part * weight
        o_lat = (o_sum / l_sum).astype(BF16)
        v_v[:, h * value:(h + 1) * value] = jnp.dot(o_lat, wuv_ref[h], preferred_element_type=F32).astype(BF16)
    out = hid_ref[...].astype(F32) + jnp.dot(v_v[...], wo_ref[...], preferred_element_type=F32)
    out_ref[...] = out.astype(BF16)


def finish_output(hidden, w_uv, w_o, suffix, parts, log2_scale):
    return pl.pallas_call(
        functools.partial(output_kernel, log2_scale),
        out_shape=jax.ShapeDtypeStruct(hidden.shape, BF16),
        in_specs=[vmem()] * 12,
        out_specs=vmem(),
        scratch_shapes=[pltpu.VMEM((hidden.shape[0], w_o.shape[0]), BF16)],
        compiler_params=pltpu.CompilerParams(vmem_limit_bytes=32 * MIB),
        name='output',
    )(hidden, w_uv, w_o, *suffix, *parts)


def solution(mesh):
    group = mesh.shape['ctx']
    rows_spec = P(('dp', 'ctx'), None)
    whole_spec = P()
    over_x = [(i, i ^ 2) for i in range(group)]
    over_y = [(i, i ^ 4) for i in range(group)]

    def local_step(hidden, w_q, w_uk, w_uv, w_o, kv_prefix, kv_suffix, seq_lens):
        lat = w_uk.shape[2]
        n_head = w_uk.shape[0]
        log2_scale = LOG2E * (w_q.shape[1] // n_head) ** -0.5
        kv_own = kv_prefix.swapaxes(0, 1)
        queries, q_seq, kv_sib = make_queries(hidden, w_q, w_uk, kv_own, seq_lens, kv_prefix.shape[0] * group)
        blocks = queries.reshape(8, -1, queries.shape[-1])
        part = functools.partial(prefix_part, blocks, kv_own, kv_sib, log2_scale=log2_scale, lat=lat)
        send_x = lambda a: lax.ppermute(a, 'ctx', over_x)
        send_y = lambda a: lax.ppermute(a, 'ctx', over_y)
        da, db = part(4, 5)
        for_y, for_x = send_x(da), send_y(db)
        xa, yb = part(0, 3)
        got_xa, got_yb = send_x(xa), send_y(yb)
        oa, ob = part(6, 7)
        for_x, for_y, oa, ob = lax.optimization_barrier((for_x, for_y, oa, ob))
        xb, ya = part(1, 2, carry=(for_x, for_y))
        got_xb, got_ya = send_x(xb), send_y(ya)
        suffix = suffix_part(q_seq, kv_suffix, seq_lens, log2_scale, lat)
        return finish_output(hidden, w_uv, w_o, suffix, (oa, ob, got_xa, got_xb, got_ya, got_yb), log2_scale)

    return jax.shard_map(local_step, mesh=mesh, in_specs=(rows_spec, whole_spec, whole_spec, whole_spec, whole_spec, rows_spec, P(('dp', 'ctx'), None, None), P(('dp', 'ctx'))), out_specs=rows_spec, check_vma=False)
```

```python
import functools
import math
import jax
import jax.numpy as jnp
from jax import lax
from jax.experimental import pallas as pl
from jax.experimental.pallas import tpu as pltpu
from jax.sharding import PartitionSpec as P

ROPE_BASE = 10000
LOG2E = 1.4426950408889634
NT = (((1,), (1,)), ((), ()))
F32 = jnp.float32
BF16 = jnp.bfloat16
MIB = 1024 * 1024
TAIL = 8


def vmem():
    return pl.BlockSpec(memory_space=pltpu.VMEM)


def hbm():
    return pl.BlockSpec(memory_space=pl.ANY)


def query_kernel(n_head, nope, rope, hid_ref, trig_ref, rot_ref, wq_hbm, wuk_hbm, kv_hbm,
                 q_ref, qs_ref, kvs_hbm,
                 hid_all, trig_all, wq_v, wuk_v, qs_f, wq_sem, wuk_sem, send_sem, recv_sem):
    rows = hid_ref.shape[0]
    lat = wuk_v.shape[2]
    qk = nope + rope
    per = 4
    groups = n_head // per
    width = per * qk
    me = lax.axis_index('ctx')
    core = lax.rem(me, 2)
    xx = lax.rem(me // 2, 2)
    yy = me // 4
    sib = me + 1 - 2 * core
    to_x = me + 2 - 4 * xx
    to_y = me + 4 - 8 * yy
    to_d = me + 6 - 4 * xx - 8 * yy
    weights = []
    for g in range(groups):
        cols = pl.ds(g * width, width)
        copy = pltpu.make_async_copy(wq_hbm.at[:, cols], wq_v.at[:, cols], wq_sem.at[g])
        copy.start()
        weights.append(copy)
    wuk_copy = pltpu.make_async_copy(wuk_hbm, wuk_v, wuk_sem)
    wuk_copy.start()

    barrier = pltpu.get_barrier_semaphore()
    for peer in (sib, to_x, to_y, to_d):
        pl.semaphore_signal(barrier, inc=1, device_id={'ctx': peer})
    pl.semaphore_wait(barrier, 4)
    sends = []
    for slot, peer in ((2, to_d), (0, to_x), (1, to_y)):
        sends.append(pltpu.make_async_remote_copy(
            src_ref=hid_ref, dst_ref=hid_all.at[slot], send_sem=send_sem.at[slot], recv_sem=recv_sem.at[slot],
            device_id={'ctx': peer}))
        sends.append(pltpu.make_async_remote_copy(
            src_ref=trig_ref, dst_ref=trig_all.at[slot], send_sem=send_sem.at[3 + slot], recv_sem=recv_sem.at[3 + slot],
            device_id={'ctx': peer}))
    sends.append(pltpu.make_async_remote_copy(
        src_ref=kv_hbm, dst_ref=kvs_hbm, send_sem=send_sem.at[6], recv_sem=recv_sem.at[6], device_id={'ctx': sib}))
    for copy in sends:
        copy.start()

    def project(hid, cos, sin, g, store):
        q_all = jnp.dot(hid, wq_v[:, g * width:(g + 1) * width], preferred_element_type=F32)
        for j in range(per):
            h = g * per + j
            q_nope = q_all[:, j * qk:j * qk + nope].astype(BF16)
            q_pe = q_all[:, j * qk + nope:(j + 1) * qk].astype(BF16)
            q_lat = jnp.dot(q_nope, wuk_v[h], preferred_element_type=F32).astype(BF16)
            turned = jnp.dot(q_pe, rot_ref[...], preferred_element_type=F32)
            q_rot = (q_pe.astype(F32) * cos + turned * sin).astype(BF16)
            store(h, q_lat, q_rot)

    def store_own(h, q_lat, q_rot):
        q_ref[3, h, :, 0:lat] = q_lat
        q_ref[3, h, :, lat:lat + rope] = q_rot
        for n in range(lat // 128):
            qs_f[n, pl.ds(h, rows, stride=n_head), :] = q_lat[:, n * 128:(n + 1) * 128].astype(F32)
        wide_rot = jnp.concatenate([q_rot, q_rot], axis=1).astype(F32)
        qs_f[lat // 128, pl.ds(h, rows, stride=n_head), :] = wide_rot

    def store_peer(h, q_lat, q_rot):
        for p in range(3):
            q_ref[p, h, :, 0:lat] = q_lat[p * rows:(p + 1) * rows]
            q_ref[p, h, :, lat:lat + rope] = q_rot[p * rows:(p + 1) * rows]

    wuk_copy.wait()
    for g in range(groups):
        weights[g].wait()
        project(hid_ref[...], trig_ref[0], trig_ref[1], g, store_own)
    for n in range(lat // 128):
        qs_ref[:, n * 128:(n + 1) * 128] = qs_f[n].astype(BF16)
    qs_ref[:, lat:lat + rope] = qs_f[lat // 128][:, 0:rope].astype(BF16)
    for copy in sends[:-1]:
        copy.wait()
    hid3 = hid_all[...].reshape(3 * rows, hid_ref.shape[1])
    cos3 = jnp.concatenate([trig_all[p, 0] for p in range(3)], axis=0)
    sin3 = jnp.concatenate([trig_all[p, 1] for p in range(3)], axis=0)
    for g in range(groups):
        project(hid3, cos3, sin3, g, store_peer)
    sends[-1].wait()


def make_queries(hidden, w_q, w_uk, kv_own, seq_lens, first_pos):
    rows, dim = hidden.shape
    n_head, nope, lat = w_uk.shape
    qk = w_q.shape[1] // n_head
    rope = qk - nope
    half = rope // 2
    inv_freq = jnp.exp(jnp.arange(half, dtype=F32) * (-math.log(ROPE_BASE) / half))
    angle = (first_pos + seq_lens).astype(F32)[:, None] * inv_freq
    cos_part, sin_part = jnp.cos(angle), jnp.sin(angle)
    trig = jnp.stack([jnp.concatenate([cos_part, cos_part], -1), jnp.concatenate([sin_part, sin_part], -1)])
    i, j = jnp.arange(rope)[:, None], jnp.arange(rope)[None, :]
    rot = jnp.where(i == j + half, -1.0, jnp.where(i + half == j, 1.0, 0.0)).astype(BF16)
    return pl.pallas_call(
        functools.partial(query_kernel, n_head, nope, rope),
        out_shape=(jax.ShapeDtypeStruct((4, n_head, rows, lat + rope), BF16),
                   jax.ShapeDtypeStruct((rows * n_head, lat + rope), BF16),
                   jax.ShapeDtypeStruct(kv_own.shape, BF16)),
        in_specs=[vmem(), vmem(), vmem(), hbm(), hbm(), hbm()],
        out_specs=(vmem(), vmem(), hbm()),
        scratch_shapes=[
            pltpu.VMEM((3, rows, dim), BF16), pltpu.VMEM((3, 2, rows, rope), F32),
            pltpu.VMEM(w_q.shape, BF16), pltpu.VMEM(w_uk.shape, BF16),
            pltpu.VMEM((lat // 128 + 1, rows * n_head, 128), F32),
            pltpu.SemaphoreType.DMA((n_head // 4,)), pltpu.SemaphoreType.DMA,
            pltpu.SemaphoreType.DMA((7,)), pltpu.SemaphoreType.DMA((7,))],
        compiler_params=pltpu.CompilerParams(collective_id=0, has_side_effects=True, vmem_limit_bytes=40 * MIB),
        name='queries',
    )(hidden, trig, rot, w_q, w_uk, kv_own)


def wide(x, n):
    return jnp.concatenate([x] * n, axis=1)


def prefix_kernel(log2_scale, lat, tile, carried, *refs):
    if carried:
        qa_ref, qb_ref, ka_ref, kb_ref, ca_ref, cb_ref, oa_ref, ob_ref, q_v, m_v, l_v, acc, s_v, p_v = refs
    else:
        qa_ref, qb_ref, ka_ref, kb_ref, oa_ref, ob_ref, q_v, m_v, l_v, acc, s_v, p_v = refs
    half = qa_ref.shape[1]
    block = ka_ref.shape[1]
    step = pl.program_id(0)

    @pl.when(step == 0)
    def _():
        q_v[0:half] = qa_ref[0]
        q_v[half:] = qb_ref[0]
        if carried:
            first_lane = lax.broadcasted_iota(jnp.int32, (half, 128), 1) == 0
            for n, c_ref in enumerate((ca_ref, cb_ref)):
                at = slice(n * half, (n + 1) * half)
                acc[at] = c_ref[0:half]
                m_col = jnp.transpose(c_ref[half:half + TAIL, 0:half])[:, 0:1]
                l_col = jnp.transpose(c_ref[half:half + TAIL, half:2 * half])[:, 0:1]
                m_v[at] = jnp.broadcast_to(m_col, (half, 128))
                l_v[at] = jnp.where(first_lane, l_col, 0.0)
        else:
            acc[...] = jnp.zeros_like(acc)
            m_v[...] = jnp.full_like(m_v, -jnp.inf)
            l_v[...] = jnp.zeros_like(l_v)

    items = [(k_ref, r) for k_ref in (ka_ref, kb_ref) for r in range(0, 2 * half, tile)]
    for n, (k_ref, r) in enumerate(items):
        s_v[n] = jnp.dot(q_v[r:r + tile], k_ref[...], preferred_element_type=F32)
    for n, (k_ref, r) in enumerate(items):
        for t in range(0, tile, 64):
            at = slice(r + t, r + t + 64)
            s = s_v[n, t:t + 64]
            m_old = m_v[at]
            m_new = jnp.maximum(m_old, jnp.max(s, axis=1, keepdims=True))
            alpha = jnp.exp2((m_old - m_new) * log2_scale)
            p = jnp.exp2((s - wide(m_new, block // 128)) * log2_scale)
            part = p[:, 0:128]
            for j in range(1, block // 128):
                part += p[:, j * 128:(j + 1) * 128]
            l_v[at] = l_v[at] * alpha + part
            m_v[at] = m_new
            p_v[n, t:t + 64] = p.astype(BF16)
            acc[at] = acc[at] * wide(alpha, lat // 128)
        at = slice(r, r + tile)
        acc[at] += lax.dot_general(p_v[n], k_ref[0:lat, :], NT, preferred_element_type=F32)

    @pl.when(step == pl.num_programs(0) - 1)
    def _():
        for n, o_ref in enumerate((oa_ref, ob_ref)):
            at = slice(n * half, (n + 1) * half)
            o_ref[0:half] = acc[at]
            o_ref[half:half + TAIL, 0:half] = jnp.transpose(m_v[at])[0:TAIL]
            l_sum = jnp.broadcast_to(jnp.sum(l_v[at], axis=1, keepdims=True), (half, 128))
            o_ref[half:half + TAIL, half:2 * half] = jnp.transpose(l_sum)[0:TAIL]


def prefix_part(q_blocks, kv_own, kv_sib, pick_a, pick_b, log2_scale, lat, carry=None, block=1024, tile=512):
    half, width = q_blocks.shape[1:]
    steps = kv_own.shape[1] // block
    payload = jax.ShapeDtypeStruct((half + TAIL, lat), F32)
    whole = pl.BlockSpec((half + TAIL, lat), lambda i: (0, 0))
    keys = pl.BlockSpec((width, block), lambda i: (0, i))
    carry = () if carry is None else tuple(carry)
    flops = 2 * 2 * half * 2 * kv_own.shape[1] * (width + lat)
    items = 2 * (2 * half // tile)
    return pl.pallas_call(
        functools.partial(prefix_kernel, log2_scale, lat, tile, bool(carry)),
        grid=(steps,),
        out_shape=(payload, payload),
        in_specs=[pl.BlockSpec((1, half, width), lambda i: (pick_a, 0, 0)),
                  pl.BlockSpec((1, half, width), lambda i: (pick_b, 0, 0)), keys, keys] + [whole] * len(carry),
        out_specs=(whole, whole),
        scratch_shapes=[pltpu.VMEM((2 * half, width), BF16), pltpu.VMEM((2 * half, 128), F32),
                        pltpu.VMEM((2 * half, 128), F32), pltpu.VMEM((2 * half, lat), F32),
                        pltpu.VMEM((items, tile, block), F32), pltpu.VMEM((items, tile, block), BF16)],
        compiler_params=pltpu.CompilerParams(vmem_limit_bytes=32 * MIB),
        cost_estimate=pl.CostEstimate(flops=flops, bytes_accessed=8 * MIB, transcendentals=0),
        name='prefix',
    )(q_blocks, q_blocks, kv_own, kv_sib, *carry)


def suffix_kernel(log2_scale, lat, chunk, unit, n_buf, lens_ref, q_ref, kv_hbm, o_ref, m_ref, l_ref,
                  kv_v, s_v, p_v, a_v, m_v, l_v, acc, sems, b_s, c_s):
    n_seq = lens_ref.shape[0]
    heads = q_ref.shape[0] // n_seq
    shift = chunk.bit_length() - 1
    total = jnp.int32(0)
    for b in range(n_seq):
        total += lax.shift_right_logical(lens_ref[b], shift) + 1
    trips = lax.div(total + unit - 1, unit)
    ring = n_buf // unit
    depth = ring - 3

    def last_chunk(b):
        return lax.shift_right_logical(lens_ref[jnp.minimum(b, n_seq - 1)], shift)

    def fetch(b, c, slot):
        return pltpu.make_async_copy(
            kv_hbm.at[b, :, pl.ds(pl.multiple_of(c * chunk, chunk), chunk)], kv_v.at[slot], sems.at[slot])

    def start(at, slot):
        b, c = at
        b_s[slot] = b
        c_s[slot] = c

        @pl.when(b < n_seq)
        def _():
            fetch(b, c, slot).start()
        last = c >= last_chunk(b)
        return jnp.where(last, jnp.minimum(b + 1, n_seq), b), jnp.where(last, 0, c + 1)

    for slot in range(depth * unit, n_buf):
        b_s[slot] = n_seq
        c_s[slot] = 0
    ahead = lax.fori_loop(0, depth * unit, lambda j, at: start(at, j), (jnp.int32(0), jnp.int32(0)))

    def step(i, at):
        base, prev, back, far = [lax.rem(i + d, ring) * unit for d in (0, ring - 1, ring - 2, depth)]
        for u in range(unit):
            at = start(at, far + u)
        for u in range(unit):
            @pl.when(b_s[base + u] < n_seq)
            def _(u=u):
                fetch(0, 0, base + u).wait()

        total_o = acc[...]
        for u in range(unit):
            added = lax.dot_general(p_v[u], kv_v[back + u, 0:lat, :], NT, preferred_element_type=F32)
            kept = jnp.where(c_s[back + u] == 0, 0.0, total_o * wide(a_v[u], lat // 128))
            total_o = kept + added
            out = pl.ds(pl.multiple_of(b_s[back + u] * heads, heads), heads)
            for n in range(lat // 128):
                o_ref[n, out, :] = total_o[:, n * 128:(n + 1) * 128]
        acc[...] = total_o

        lanes = lax.broadcasted_iota(jnp.int32, (heads, chunk), 1)
        scores, tops = [], []
        for u in range(unit):
            b, c = b_s[prev + u], c_s[prev + u]
            length = lens_ref[jnp.minimum(b, n_seq - 1)]
            scores.append(jnp.where(lanes <= length - c * chunk, s_v[u], -jnp.inf))
        top = jnp.max(jnp.concatenate(scores, axis=0), axis=1, keepdims=True)
        m_old, l_old = m_v[...], l_v[...]
        for u in range(unit):
            first = c_s[prev + u] == 0
            m_old = jnp.where(first, -jnp.inf, m_old)
            m_new = jnp.maximum(m_old, top[u * heads:(u + 1) * heads])
            alpha = jnp.exp2((m_old - m_new) * log2_scale)
            p = jnp.exp2((scores[u] - wide(m_new, chunk // 128)) * log2_scale)
            part = p[:, 0:128]
            for n in range(1, chunk // 128):
                part += p[:, n * 128:(n + 1) * 128]
            l_old = jnp.where(first, 0.0, l_old * alpha) + part
            m_old = m_new
            p_v[u] = p.astype(BF16)
            a_v[u] = alpha
            out = pl.ds(pl.multiple_of(b_s[prev + u] * heads, heads), heads)
            m_ref[out, :] = m_old
            l_ref[out, :] = l_old
        m_v[...] = m_old
        l_v[...] = l_old

        for u in range(unit):
            bq = jnp.minimum(b_s[base + u], n_seq - 1)
            q = q_ref[pl.ds(pl.multiple_of(bq * heads, heads), heads), :]
            s_v[u] = jnp.dot(q, kv_v[base + u], preferred_element_type=F32)
        return at

    lax.fori_loop(0, trips + 2, step, ahead)


def suffix_part(q_seq, kv_suffix, seq_lens, log2_scale, lat, chunk=256, unit=4, n_buf=32):
    n_seq, slots, wide_row = kv_suffix.shape
    rows = q_seq.shape[0]
    heads = rows // n_seq
    flops = 2 * rows * slots * (wide_row + lat) * 4
    return pl.pallas_call(
        functools.partial(suffix_kernel, log2_scale, lat, chunk, unit, n_buf),
        out_shape=(jax.ShapeDtypeStruct((lat // 128, rows + heads, 128), F32), jax.ShapeDtypeStruct((rows + heads, 128), F32),
                   jax.ShapeDtypeStruct((rows + heads, 128), F32)),
        in_specs=[pl.BlockSpec(memory_space=pltpu.SMEM), vmem(), hbm()],
        out_specs=(vmem(), vmem(), vmem()),
        scratch_shapes=[pltpu.VMEM((n_buf, wide_row, chunk), BF16), pltpu.VMEM((unit, heads, chunk), F32),
                        pltpu.VMEM((unit, heads, chunk), BF16), pltpu.VMEM((unit, heads, 128), F32),
                        pltpu.VMEM((heads, 128), F32), pltpu.VMEM((heads, 128), F32),
                        pltpu.VMEM((heads, lat), F32), pltpu.SemaphoreType.DMA((n_buf,)),
                        pltpu.SMEM((n_buf,), jnp.int32), pltpu.SMEM((n_buf,), jnp.int32)],
        compiler_params=pltpu.CompilerParams(vmem_limit_bytes=32 * MIB),
        cost_estimate=pl.CostEstimate(flops=flops, bytes_accessed=40 * MIB, transcendentals=0),
        name='suffix',
    )(seq_lens, q_seq, kv_suffix.swapaxes(1, 2))


def output_kernel(log2_scale, hid_ref, wuv_ref, wo_ref, so_ref, sm_ref, sl_ref, *refs):
    parts, out_ref, v_v = refs[:6], refs[6], refs[7]
    n_head = wuv_ref.shape[0]
    rows = hid_ref.shape[0]
    half = n_head // 2
    block = half * rows
    value = wuv_ref.shape[2]
    cols = []
    for part in parts:
        m_t = jnp.transpose(part[block:block + TAIL, 0:block])
        l_t = jnp.transpose(part[block:block + TAIL, block:2 * block])
        cols.append((m_t[:, 0:1], l_t[:, 0:1]))
    for h in range(n_head):
        side, at = h // half, (h % half) * rows
        mine = pl.ds(h, rows, stride=n_head)
        own = jnp.concatenate([so_ref[n, mine, :] for n in range(so_ref.shape[0])], axis=1)
        terms = [(own, sm_ref[mine, :][:, 0:1], jnp.sum(sl_ref[mine, :], axis=1, keepdims=True))]
        for n in range(side, 6, 2):
            terms.append((parts[n][at:at + rows, :], cols[n][0][at:at + rows], cols[n][1][at:at + rows]))
        m_all = functools.reduce(jnp.maximum, [t[1] for t in terms])
        o_sum, l_sum = 0.0, 0.0
        for o_part, m_part, l_part in terms:
            weight = jnp.exp2((m_part - m_all) * log2_scale)
            o_sum += o_part * weight
            l_sum += l_part * weight
        o_lat = (o_sum / l_sum).astype(BF16)
        v_v[:, h * value:(h + 1) * value] = jnp.dot(o_lat, wuv_ref[h], preferred_element_type=F32).astype(BF16)
    out = hid_ref[...].astype(F32) + jnp.dot(v_v[...], wo_ref[...], preferred_element_type=F32)
    out_ref[...] = out.astype(BF16)


def finish_output(hidden, w_uv, w_o, suffix, parts, log2_scale):
    return pl.pallas_call(
        functools.partial(output_kernel, log2_scale),
        out_shape=jax.ShapeDtypeStruct(hidden.shape, BF16),
        in_specs=[vmem()] * 12,
        out_specs=vmem(),
        scratch_shapes=[pltpu.VMEM((hidden.shape[0], w_o.shape[0]), BF16)],
        compiler_params=pltpu.CompilerParams(vmem_limit_bytes=32 * MIB),
        name='output',
    )(hidden, w_uv, w_o, *suffix, *parts)


def solution(mesh):
    group = mesh.shape['ctx']
    rows_spec = P(('dp', 'ctx'), None)
    whole_spec = P()
    over_x = [(i, i ^ 2) for i in range(group)]
    over_y = [(i, i ^ 4) for i in range(group)]

    def local_step(hidden, w_q, w_uk, w_uv, w_o, kv_prefix, kv_suffix, seq_lens):
        lat = w_uk.shape[2]
        n_head = w_uk.shape[0]
        log2_scale = LOG2E * (w_q.shape[1] // n_head) ** -0.5
        kv_own = kv_prefix.swapaxes(0, 1)
        queries, q_seq, kv_sib = make_queries(hidden, w_q, w_uk, kv_own, seq_lens, kv_prefix.shape[0] * group)
        blocks = queries.reshape(8, -1, queries.shape[-1])
        part = functools.partial(prefix_part, blocks, kv_own, kv_sib, log2_scale=log2_scale, lat=lat)
        send_x = lambda a: lax.ppermute(a, 'ctx', over_x)
        send_y = lambda a: lax.ppermute(a, 'ctx', over_y)
        da, db = part(4, 5)
        for_y, for_x = send_x(da), send_y(db)
        xa, yb = part(0, 3)
        got_xa, got_yb = send_x(xa), send_y(yb)
        oa, ob = part(6, 7)
        for_x, for_y, oa, ob = lax.optimization_barrier((for_x, for_y, oa, ob))
        xb, ya = part(1, 2, carry=(for_x, for_y))
        got_xb, got_ya = send_x(xb), send_y(ya)
        suffix = suffix_part(q_seq, kv_suffix, seq_lens, log2_scale, lat)
        return finish_output(hidden, w_uv, w_o, suffix, (oa, ob, got_xa, got_xb, got_ya, got_yb), log2_scale)

    return jax.shard_map(local_step, mesh=mesh, in_specs=(rows_spec, whole_spec, whole_spec, whole_spec, whole_spec, rows_spec, P(('dp', 'ctx'), None, None), P(('dp', 'ctx'))), out_specs=rows_spec, check_vma=False)
```

```python
import functools
import math
import jax
import jax.numpy as jnp
from jax import lax
from jax.experimental import pallas as pl
from jax.experimental.pallas import tpu as pltpu
from jax.sharding import PartitionSpec as P

ROPE_BASE = 10000
LOG2E = 1.4426950408889634
NT = (((1,), (1,)), ((), ()))
F32 = jnp.float32
BF16 = jnp.bfloat16
MIB = 1024 * 1024
TAIL = 8


def vmem():
    return pl.BlockSpec(memory_space=pltpu.VMEM)


def hbm():
    return pl.BlockSpec(memory_space=pl.ANY)


def wide(x, n):
    return jnp.concatenate([x] * n, axis=1)


def prefix_kernel(n_head, nope, rope, log2_scale, hid_ref, cos_ref, sin_ref, wq_hbm, wuk_hbm, kv_hbm,
                  qs_ref, own_ref, x_ref, y_ref,
                  hid_all, cos_all, sin_all, wq_v, wuk_v, kv_v, q_v, qs_f, m_v, l_v, s_v, p_v, diag, carry,
                  wq_sem, own_sem, send_sem, recv_sem):
    rows = hid_ref.shape[0]
    lat = wuk_v.shape[2]
    qk = nope + rope
    per = 4
    groups = n_head // per
    width = per * qk
    half = n_head // 2
    block = half * rows
    chunk = s_v.shape[2]
    me = lax.axis_index('ctx')
    core = lax.rem(me, 2)
    xx = lax.rem(me // 2, 2)
    yy = me // 4
    sib = me + 1 - 2 * core
    to_x = me + 2 - 4 * xx
    to_y = me + 4 - 8 * yy
    to_d = me + 6 - 4 * xx - 8 * yy
    weights = []
    for g in range(groups):
        cols = pl.ds(g * width, width)
        weights.append(pltpu.make_async_copy(wq_hbm.at[:, cols], wq_v.at[:, cols], wq_sem.at[g]))
    wuk_copy = pltpu.make_async_copy(wuk_hbm, wuk_v, own_sem.at[0])
    kv_copy = pltpu.make_async_copy(kv_hbm, kv_v.at[0], own_sem.at[1])
    for copy in (weights[0], wuk_copy, *weights[1:], kv_copy):
        copy.start()

    barrier = pltpu.get_barrier_semaphore()
    for peer in (sib, to_x, to_y, to_d):
        pl.semaphore_signal(barrier, inc=1, device_id={'ctx': peer})
    pl.semaphore_wait(barrier, 4)

    def remote(src, dst, n, peer):
        return pltpu.make_async_remote_copy(
            src_ref=src, dst_ref=dst, send_sem=send_sem.at[n], recv_sem=recv_sem.at[n], device_id={'ctx': peer})

    gathers = []
    for slot, peer in ((2, to_d), (0, to_x), (1, to_y)):
        gathers.append(remote(hid_ref, hid_all.at[slot], slot, peer))
        gathers.append(remote(cos_ref, cos_all.at[slot], 3 + slot, peer))
        gathers.append(remote(sin_ref, sin_all.at[slot], 6 + slot, peer))
    kv_send = remote(kv_hbm, kv_v.at[1], 9, sib)
    for copy in (*gathers, kv_send):
        copy.start()

    i = lax.broadcasted_iota(jnp.int32, (rope, rope), 0)
    j = lax.broadcasted_iota(jnp.int32, (rope, rope), 1)
    rot = jnp.where(i == j + rope // 2, -1.0, jnp.where(i + rope // 2 == j, 1.0, 0.0)).astype(BF16)

    def project(hid, cos, sin, g, store):
        q_all = jnp.dot(hid, wq_v[:, g * width:(g + 1) * width], preferred_element_type=F32)
        for n in range(per):
            q_nope = q_all[:, n * qk:n * qk + nope].astype(BF16)
            q_pe = q_all[:, n * qk + nope:(n + 1) * qk].astype(BF16)
            q_lat = jnp.dot(q_nope, wuk_v[g * per + n], preferred_element_type=F32).astype(BF16)
            turned = jnp.dot(q_pe, rot, preferred_element_type=F32)
            q_rot = (q_pe.astype(F32) * wide(cos, 2) + turned * wide(sin, 2)).astype(BF16)
            store(g * per + n, q_lat, q_rot)

    def keep(peer, h, q_lat, q_rot):
        at = slice((h % half) * rows, (h % half + 1) * rows)
        q_v[2 * peer + h // half, at, 0:lat] = q_lat
        q_v[2 * peer + h // half, at, lat:lat + rope] = q_rot

    def store_own(h, q_lat, q_rot):
        keep(3, h, q_lat, q_rot)
        for n in range(lat // 128):
            qs_f[n, pl.ds(h, rows, stride=n_head), :] = q_lat[:, n * 128:(n + 1) * 128].astype(F32)
        qs_f[lat // 128, pl.ds(h, rows, stride=n_head), :] = wide(q_rot, 2).astype(F32)

    def store_peer(h, q_lat, q_rot):
        for p in range(3):
            keep(p, h, q_lat[p * rows:(p + 1) * rows], q_rot[p * rows:(p + 1) * rows])

    def attend(peer, o_ref):
        for n in range(2):
            o_ref[n, 0:block] = jnp.zeros((block, lat), F32)
            m_v[2 * peer + n] = jnp.full((block, 128), -jnp.inf, F32)
            l_v[2 * peer + n] = jnp.zeros((block, 128), F32)

        def visit(i, _):
            keys = pl.ds(pl.multiple_of(i * chunk, chunk), chunk)
            items = [(k, n) for k in range(2) for n in range(2)]
            for t, (k, n) in enumerate(items):
                s_v[t] = jnp.dot(q_v[2 * peer + n], kv_v[k, :, keys], preferred_element_type=F32)
            for t, (k, n) in enumerate(items):
                b = 2 * peer + n
                for r in range(0, block, 64):
                    at = slice(r, r + 64)
                    s = s_v[t, at]
                    m_old = m_v[b, at]
                    m_new = jnp.maximum(m_old, jnp.max(s, axis=1, keepdims=True))
                    alpha = jnp.exp2((m_old - m_new) * log2_scale)
                    p = jnp.exp2((s - wide(m_new, chunk // 128)) * log2_scale)
                    part = p[:, 0:128]
                    for c in range(1, chunk // 128):
                        part += p[:, c * 128:(c + 1) * 128]
                    l_v[b, at] = l_v[b, at] * alpha + part
                    m_v[b, at] = m_new
                    p_v[t, at] = p.astype(BF16)
                    o_ref[n, at] = o_ref[n, at] * wide(alpha, lat // 128)
                o_ref[n, 0:block] += lax.dot_general(p_v[t], kv_v[k, 0:lat, keys], NT, preferred_element_type=F32)
            return 0

        lax.fori_loop(0, kv_v.shape[2] // chunk, visit, 0)

    def close(peer, o_ref):
        for n in range(2):
            b = 2 * peer + n
            o_ref[n, block:block + TAIL, 0:block] = jnp.transpose(m_v[b])[0:TAIL]
            l_sum = jnp.broadcast_to(jnp.sum(l_v[b], axis=1, keepdims=True), (block, 128))
            o_ref[n, block:block + TAIL, block:2 * block] = jnp.transpose(l_sum)[0:TAIL]

    def merge(peer, n, o_ref, c):
        b = 2 * peer + n
        m_in = jnp.broadcast_to(jnp.transpose(carry[c, block:block + TAIL, 0:block])[:, 0:1], (block, 128))
        l_in = jnp.transpose(carry[c, block:block + TAIL, block:2 * block])[:, 0:1]
        m_new = jnp.maximum(m_v[b], m_in)
        mine = jnp.exp2((m_v[b] - m_new) * log2_scale)
        theirs = jnp.exp2((m_in - m_new) * log2_scale)
        first_lane = lax.broadcasted_iota(jnp.int32, (block, 128), 1) == 0
        l_v[b] = l_v[b] * mine + jnp.where(first_lane, l_in * theirs, 0.0)
        m_v[b] = m_new
        o_ref[n, 0:block] = o_ref[n, 0:block] * wide(mine, lat // 128) + carry[c, 0:block] * wide(theirs, lat // 128)

    for g in range(groups):
        weights[g].wait()
        if g == 0:
            wuk_copy.wait()
        project(hid_ref[...], cos_ref[...], sin_ref[...], g, store_own)
    for n in range(lat // 128):
        qs_ref[:, n * 128:(n + 1) * 128] = qs_f[n].astype(BF16)
    qs_ref[:, lat:lat + rope] = qs_f[lat // 128][:, 0:rope].astype(BF16)
    kv_copy.wait()
    kv_send.wait()
    attend(3, own_ref)
    close(3, own_ref)

    for copy in gathers:
        copy.wait()
    hid3 = hid_all[...].reshape(3 * rows, hid_ref.shape[1])
    cos3 = jnp.concatenate([cos_all[p] for p in range(3)], axis=0)
    sin3 = jnp.concatenate([sin_all[p] for p in range(3)], axis=0)
    for g in range(groups):
        project(hid3, cos3, sin3, g, store_peer)

    attend(2, diag)
    close(2, diag)
    over = [remote(diag.at[0], carry.at[0], 10, to_x), remote(diag.at[1], carry.at[1], 11, to_y)]
    for copy in over:
        copy.start()
    attend(0, x_ref)
    attend(1, y_ref)
    for copy in over:
        copy.wait()
    merge(1, 0, y_ref, 0)
    merge(0, 1, x_ref, 1)
    close(0, x_ref)
    close(1, y_ref)


def prefix_phase(hidden, w_q, w_uk, kv_own, seq_lens, first_pos, log2_scale, chunk=1024):
    rows, dim = hidden.shape
    n_head, nope, lat = w_uk.shape
    qk = w_q.shape[1] // n_head
    rope = qk - nope
    inv_freq = jnp.exp(jnp.arange(rope // 2, dtype=F32) * (-math.log(ROPE_BASE) / (rope // 2)))
    angle = (first_pos + seq_lens).astype(F32)[:, None] * inv_freq
    block = n_head // 2 * rows
    payload = jax.ShapeDtypeStruct((2, block + TAIL, lat), F32)
    in_hbm = pl.BlockSpec(memory_space=pltpu.HBM)
    return pl.pallas_call(
        functools.partial(prefix_kernel, n_head, nope, rope, log2_scale),
        out_shape=(jax.ShapeDtypeStruct((rows * n_head, lat + rope), BF16), payload, payload, payload),
        in_specs=[vmem(), vmem(), vmem(), in_hbm, in_hbm, in_hbm],
        out_specs=(vmem(), vmem(), vmem(), vmem()),
        scratch_shapes=[
            pltpu.VMEM((3, rows, dim), BF16), pltpu.VMEM((3, rows, rope // 2), F32), pltpu.VMEM((3, rows, rope // 2), F32),
            pltpu.VMEM(w_q.shape, BF16), pltpu.VMEM(w_uk.shape, BF16), pltpu.VMEM((2, *kv_own.shape), BF16),
            pltpu.VMEM((8, block, lat + rope), BF16), pltpu.VMEM((lat // 128 + 1, rows * n_head, 128), F32),
            pltpu.VMEM((8, block, 128), F32), pltpu.VMEM((8, block, 128), F32),
            pltpu.VMEM((4, block, chunk), F32), pltpu.VMEM((4, block, chunk), BF16),
            pltpu.VMEM(payload.shape, F32), pltpu.VMEM(payload.shape, F32),
            pltpu.SemaphoreType.DMA((n_head // 4,)), pltpu.SemaphoreType.DMA((2,)),
            pltpu.SemaphoreType.DMA((12,)), pltpu.SemaphoreType.DMA((12,))],
        compiler_params=pltpu.CompilerParams(collective_id=0, has_side_effects=True, vmem_limit_bytes=60 * MIB),
        name='prefix',
    )(hidden, jnp.cos(angle), jnp.sin(angle), w_q, w_uk, kv_own)


def suffix_kernel(log2_scale, lat, chunk, unit, ring, lens_ref, q_ref, kv_hbm, o_ref, m_ref, l_ref,
                  kv_v, s_v, m_v, l_v, acc, sems, b_s, c_s):
    n_seq = lens_ref.shape[0]
    heads = q_ref.shape[0] // n_seq
    shift = chunk.bit_length() - 1
    total = jnp.int32(0)
    for b in range(n_seq):
        total += lax.shift_right_logical(lens_ref[b], shift) + 1
    trips = lax.div(total + unit - 1, unit)
    depth = ring - 2

    def start(at, group):
        b, c = at
        for u in range(unit):
            b_s[group * unit + u] = b
            c_s[group * unit + u] = c
            have = jnp.minimum(b, n_seq - 1)
            pltpu.make_async_copy(
                kv_hbm.at[have, :, pl.ds(pl.multiple_of(c * chunk, chunk), chunk)], kv_v.at[group, u], sems.at[group]).start()
            last = c >= lax.shift_right_logical(lens_ref[have], shift)
            b, c = jnp.where(last, jnp.minimum(b + 1, n_seq), b), jnp.where(last, 0, c + 1)
        return b, c

    for u in range(unit):
        b_s[(ring - 1) * unit + u] = n_seq
        c_s[(ring - 1) * unit + u] = 0
    ahead = lax.fori_loop(0, jnp.minimum(depth, trips), lambda j, at: start(at, j), (jnp.int32(0), jnp.int32(0)))

    def step(i, at):
        base, prev, far = [lax.rem(i + d, ring) for d in (0, ring - 1, depth)]
        at = lax.cond(i + depth < trips, lambda: start(at, far), lambda: at)

        @pl.when(i < trips)
        def _():
            pltpu.make_async_copy(kv_v.at[base], kv_v.at[base], sems.at[base]).wait()

        here, there = lax.rem(i, 2), lax.rem(i + 1, 2)
        for u in range(unit):
            bq = jnp.minimum(b_s[base * unit + u], n_seq - 1)
            q = q_ref[pl.ds(pl.multiple_of(bq * heads, heads), heads), :]
            s_v[here, u] = jnp.dot(q, kv_v[base, u], preferred_element_type=F32)

        lanes = lax.broadcasted_iota(jnp.int32, (heads, chunk), 1)
        items = [(b_s[prev * unit + u], c_s[prev * unit + u]) for u in range(unit)]
        scores = []
        for u, (b, c) in enumerate(items):
            length = lens_ref[jnp.minimum(b, n_seq - 1)]
            scores.append(jnp.where(lanes <= length - c * chunk, s_v[there, u], -jnp.inf))
        top = jnp.max(jnp.concatenate(scores, axis=0), axis=1, keepdims=True)
        m_old, l_old, o_old = m_v[...], l_v[...], acc[...]
        for u, (b, c) in enumerate(items):
            first = c == 0
            m_old = jnp.where(first, -jnp.inf, m_old)
            m_new = jnp.maximum(m_old, top[u * heads:(u + 1) * heads])
            alpha = jnp.exp2((m_old - m_new) * log2_scale)
            p = jnp.exp2((scores[u] - wide(m_new, chunk // 128)) * log2_scale)
            part = p[:, 0:128]
            for n in range(1, chunk // 128):
                part += p[:, n * 128:(n + 1) * 128]
            added = lax.dot_general(p.astype(BF16), kv_v[prev, u, 0:lat, :], NT, preferred_element_type=F32)
            l_old = jnp.where(first, 0.0, l_old * alpha) + part
            o_old = jnp.where(first, 0.0, o_old * wide(alpha, lat // 128)) + added
            m_old = m_new
            out = pl.ds(pl.multiple_of(b * heads, heads), heads)
            m_ref[out, :] = m_old
            l_ref[out, :] = l_old
            for n in range(lat // 128):
                o_ref[n, out, :] = o_old[:, n * 128:(n + 1) * 128]
        m_v[...], l_v[...], acc[...] = m_old, l_old, o_old
        return at

    lax.fori_loop(0, trips + 1, step, ahead)


def suffix_part(q_seq, kv_suffix, seq_lens, log2_scale, lat, chunk=256, unit=8, ring=5):
    n_seq, slots, wide_row = kv_suffix.shape
    rows = q_seq.shape[0]
    heads = rows // n_seq
    flops = 2 * rows * slots * (wide_row + lat) * 4
    return pl.pallas_call(
        functools.partial(suffix_kernel, log2_scale, lat, chunk, unit, ring),
        out_shape=(jax.ShapeDtypeStruct((lat // 128, rows + heads, 128), F32), jax.ShapeDtypeStruct((rows + heads, 128), F32),
                   jax.ShapeDtypeStruct((rows + heads, 128), F32)),
        in_specs=[pl.BlockSpec(memory_space=pltpu.SMEM), vmem(), hbm()],
        out_specs=(vmem(), vmem(), vmem()),
        scratch_shapes=[pltpu.VMEM((ring, unit, wide_row, chunk), BF16), pltpu.VMEM((2, unit, heads, chunk), F32),
                        pltpu.VMEM((heads, 128), F32), pltpu.VMEM((heads, 128), F32),
                        pltpu.VMEM((heads, lat), F32), pltpu.SemaphoreType.DMA((ring,)),
                        pltpu.SMEM((ring * unit,), jnp.int32), pltpu.SMEM((ring * unit,), jnp.int32)],
        compiler_params=pltpu.CompilerParams(vmem_limit_bytes=32 * MIB),
        cost_estimate=pl.CostEstimate(flops=flops, bytes_accessed=40 * MIB, transcendentals=0),
        name='suffix',
    )(seq_lens, q_seq, kv_suffix.swapaxes(1, 2))


def output_kernel(log2_scale, hid_ref, wuv_ref, wo_ref, so_ref, sm_ref, sl_ref, own_ref, x_ref, y_ref, out_ref, v_v):
    n_head = wuv_ref.shape[0]
    rows = hid_ref.shape[0]
    half = n_head // 2
    block = half * rows
    value = wuv_ref.shape[2]
    parts = [[(own_ref, n), (x_ref, n), (y_ref, n)] for n in range(2)]
    cols = []
    for side in parts:
        for ref, n in side:
            m_t = jnp.transpose(ref[n, block:block + TAIL, 0:block])
            l_t = jnp.transpose(ref[n, block:block + TAIL, block:2 * block])
            cols.append((m_t[:, 0:1], l_t[:, 0:1]))
    for h in range(n_head):
        side, at = h // half, (h % half) * rows
        mine = pl.ds(h, rows, stride=n_head)
        own = jnp.concatenate([so_ref[n, mine, :] for n in range(so_ref.shape[0])], axis=1)
        terms = [(own, sm_ref[mine, :][:, 0:1], jnp.sum(sl_ref[mine, :], axis=1, keepdims=True))]
        for k, (ref, n) in enumerate(parts[side]):
            m_part, l_part = cols[side * 3 + k]
            terms.append((ref[n, at:at + rows, :], m_part[at:at + rows], l_part[at:at + rows]))
        m_all = functools.reduce(jnp.maximum, [t[1] for t in terms])
        o_sum, l_sum = 0.0, 0.0
        for o_part, m_part, l_part in terms:
            weight = jnp.exp2((m_part - m_all) * log2_scale)
            o_sum += o_part * weight
            l_sum += l_part * weight
        o_lat = (o_sum / l_sum).astype(BF16)
        v_v[:, h * value:(h + 1) * value] = jnp.dot(o_lat, wuv_ref[h], preferred_element_type=F32).astype(BF16)
    out = hid_ref[...].astype(F32) + jnp.dot(v_v[...], wo_ref[...], preferred_element_type=F32)
    out_ref[...] = out.astype(BF16)


def finish_output(hidden, w_uv, w_o, suffix, parts, log2_scale):
    return pl.pallas_call(
        functools.partial(output_kernel, log2_scale),
        out_shape=jax.ShapeDtypeStruct(hidden.shape, BF16),
        in_specs=[vmem()] * 9,
        out_specs=vmem(),
        scratch_shapes=[pltpu.VMEM((hidden.shape[0], w_o.shape[0]), BF16)],
        compiler_params=pltpu.CompilerParams(vmem_limit_bytes=32 * MIB),
        name='output',
    )(hidden, w_uv, w_o, *suffix, *parts)


def solution(mesh):
    group = mesh.shape['ctx']
    rows_spec = P(('dp', 'ctx'), None)
    whole_spec = P()
    over_x = [(i, i ^ 2) for i in range(group)]
    over_y = [(i, i ^ 4) for i in range(group)]

    def local_step(hidden, w_q, w_uk, w_uv, w_o, kv_prefix, kv_suffix, seq_lens):
        lat = w_uk.shape[2]
        n_head = w_uk.shape[0]
        log2_scale = LOG2E * (w_q.shape[1] // n_head) ** -0.5
        kv_own = kv_prefix.swapaxes(0, 1)
        q_seq, own, to_x, to_y = prefix_phase(hidden, w_q, w_uk, kv_own, seq_lens, kv_prefix.shape[0] * group, log2_scale)
        got_x, got_y = lax.ppermute(to_x, 'ctx', over_x), lax.ppermute(to_y, 'ctx', over_y)
        suffix = suffix_part(q_seq, kv_suffix, seq_lens, log2_scale, lat)
        return finish_output(hidden, w_uv, w_o, suffix, (own, got_x, got_y), log2_scale)

    return jax.shard_map(local_step, mesh=mesh, in_specs=(rows_spec, whole_spec, whole_spec, whole_spec, whole_spec, rows_spec, P(('dp', 'ctx'), None, None), P(('dp', 'ctx'))), out_specs=rows_spec, check_vma=False)
```

```python
import functools
import math
import jax
import jax.numpy as jnp
from jax import lax
from jax.experimental import pallas as pl
from jax.experimental.pallas import tpu as pltpu
from jax.sharding import PartitionSpec as P

ROPE_BASE = 10000
LOG2E = 1.4426950408889634
NT = (((1,), (1,)), ((), ()))
F32 = jnp.float32
BF16 = jnp.bfloat16
MIB = 1024 * 1024
TAIL = 8


def vmem():
    return pl.BlockSpec(memory_space=pltpu.VMEM)


def hbm():
    return pl.BlockSpec(memory_space=pl.ANY)


def wide(x, n):
    return jnp.concatenate([x] * n, axis=1)


def prefix_kernel(n_head, nope, rope, log2_scale, hid_ref, cos_ref, sin_ref, wq_hbm, wuk_hbm, kv_hbm,
                  qs_hbm, own_hbm, x_hbm, y_hbm, soon_x_hbm, soon_y_hbm,
                  hid_all, cos_all, sin_all, wq_v, wuk_v, kv_v, q_v, qs_f, qs_v, m_v, l_v, s_v, p_v,
                  own_v, x_v, y_v, diag, carry, wq_sem, own_sem, out_sem, send_sem, recv_sem):
    rows = hid_ref.shape[0]
    lat = wuk_v.shape[2]
    qk = nope + rope
    per = 4
    groups = n_head // per
    width = per * qk
    half = n_head // 2
    block = half * rows
    chunk = s_v.shape[2]
    soon = soon_x_hbm.shape[0]
    rest = block + TAIL - soon
    me = lax.axis_index('ctx')
    core = lax.rem(me, 2)
    xx = lax.rem(me // 2, 2)
    yy = me // 4
    sib = me + 1 - 2 * core
    to_x = me + 2 - 4 * xx
    to_y = me + 4 - 8 * yy
    to_d = me + 6 - 4 * xx - 8 * yy
    weights = []
    for g in range(groups):
        cols = pl.ds(g * width, width)
        weights.append(pltpu.make_async_copy(wq_hbm.at[:, cols], wq_v.at[:, cols], wq_sem.at[g]))
    wuk_copy = pltpu.make_async_copy(wuk_hbm, wuk_v, own_sem.at[0])
    kv_copy = pltpu.make_async_copy(kv_hbm, kv_v.at[0], own_sem.at[1])
    for copy in (weights[0], wuk_copy, *weights[1:], kv_copy):
        copy.start()

    barrier = pltpu.get_barrier_semaphore()
    for peer in (sib, to_x, to_y, to_d):
        pl.semaphore_signal(barrier, inc=1, device_id={'ctx': peer})
    pl.semaphore_wait(barrier, 4)

    def remote(src, dst, n, peer):
        return pltpu.make_async_remote_copy(
            src_ref=src, dst_ref=dst, send_sem=send_sem.at[n], recv_sem=recv_sem.at[n], device_id={'ctx': peer})

    gathers = []
    for slot, peer in ((2, to_d), (0, to_x), (1, to_y)):
        gathers.append(remote(hid_ref, hid_all.at[slot], slot, peer))
        gathers.append(remote(cos_ref, cos_all.at[slot], 3 + slot, peer))
        gathers.append(remote(sin_ref, sin_all.at[slot], 6 + slot, peer))
    kv_send = remote(kv_hbm, kv_v.at[1], 9, sib)
    for copy in (*gathers, kv_send):
        copy.start()

    i = lax.broadcasted_iota(jnp.int32, (rope, rope), 0)
    j = lax.broadcasted_iota(jnp.int32, (rope, rope), 1)
    rot = jnp.where(i == j + rope // 2, -1.0, jnp.where(i + rope // 2 == j, 1.0, 0.0)).astype(BF16)

    def project(hid, cos, sin, g, store):
        q_all = jnp.dot(hid, wq_v[:, g * width:(g + 1) * width], preferred_element_type=F32)
        for n in range(per):
            q_nope = q_all[:, n * qk:n * qk + nope].astype(BF16)
            q_pe = q_all[:, n * qk + nope:(n + 1) * qk].astype(BF16)
            q_lat = jnp.dot(q_nope, wuk_v[g * per + n], preferred_element_type=F32).astype(BF16)
            turned = jnp.dot(q_pe, rot, preferred_element_type=F32)
            q_rot = (q_pe.astype(F32) * wide(cos, 2) + turned * wide(sin, 2)).astype(BF16)
            store(g * per + n, q_lat, q_rot)

    def keep(peer, h, q_lat, q_rot):
        at = slice((h % half) * rows, (h % half + 1) * rows)
        q_v[2 * peer + h // half, at, 0:lat] = q_lat
        q_v[2 * peer + h // half, at, lat:lat + rope] = q_rot

    def store_own(h, q_lat, q_rot):
        keep(3, h, q_lat, q_rot)
        for n in range(lat // 128):
            qs_f[n, pl.ds(h, rows, stride=n_head), :] = q_lat[:, n * 128:(n + 1) * 128].astype(F32)
        qs_f[lat // 128, pl.ds(h, rows, stride=n_head), :] = wide(q_rot, 2).astype(F32)

    def store_peer(h, q_lat, q_rot):
        for p in range(3):
            keep(p, h, q_lat[p * rows:(p + 1) * rows], q_rot[p * rows:(p + 1) * rows])

    def attend(targets, between=()):
        for b, o_ref, n in targets:
            o_ref[n, 0:block] = jnp.zeros((block, lat), F32)
            m_v[b] = jnp.full((block, 128), -jnp.inf, F32)
            l_v[b] = jnp.zeros((block, 128), F32)
        for copy in between:
            copy.start()

        def visit(i, _):
            keys = pl.ds(pl.multiple_of(i * chunk, chunk), chunk)
            items = [(k, *target) for k in range(2) for target in targets]
            def score(t):
                k, b = items[t][:2]
                s_v[t] = jnp.dot(q_v[b], kv_v[k, :, keys], preferred_element_type=F32)

            score(0)
            for t, (k, b, o_ref, n) in enumerate(items):
                if t + 1 < len(items):
                    score(t + 1)
                for r in range(0, block, 64):
                    at = slice(r, r + 64)
                    s = s_v[t, at]
                    m_old = m_v[b, at]
                    m_new = jnp.maximum(m_old, jnp.max(s, axis=1, keepdims=True))
                    alpha = jnp.exp2((m_old - m_new) * log2_scale)
                    p = jnp.exp2((s - wide(m_new, chunk // 128)) * log2_scale)
                    part = p[:, 0:128]
                    for c in range(1, chunk // 128):
                        part += p[:, c * 128:(c + 1) * 128]
                    l_v[b, at] = l_v[b, at] * alpha + part
                    m_v[b, at] = m_new
                    p_v[t, at] = p.astype(BF16)
                    o_ref[n, at] = o_ref[n, at] * wide(alpha, lat // 128)
                o_ref[n, 0:block] += lax.dot_general(p_v[t], kv_v[k, 0:lat, keys], NT, preferred_element_type=F32)
            return 0

        lax.fori_loop(0, kv_v.shape[2] // chunk, visit, 0)

    def close(targets):
        for b, o_ref, n in targets:
            o_ref[n, block:block + TAIL, 0:block] = jnp.transpose(m_v[b])[0:TAIL]
            l_sum = jnp.broadcast_to(jnp.sum(l_v[b], axis=1, keepdims=True), (block, 128))
            o_ref[n, block:block + TAIL, block:2 * block] = jnp.transpose(l_sum)[0:TAIL]

    def merge(b, o_ref, n, c):
        m_in = jnp.broadcast_to(jnp.transpose(carry[c, block:block + TAIL, 0:block])[:, 0:1], (block, 128))
        l_in = jnp.transpose(carry[c, block:block + TAIL, block:2 * block])[:, 0:1]
        m_new = jnp.maximum(m_v[b], m_in)
        mine = jnp.exp2((m_v[b] - m_new) * log2_scale)
        theirs = jnp.exp2((m_in - m_new) * log2_scale)
        first_lane = lax.broadcasted_iota(jnp.int32, (block, 128), 1) == 0
        l_v[b] = l_v[b] * mine + jnp.where(first_lane, l_in * theirs, 0.0)
        m_v[b] = m_new
        o_ref[n, 0:block] = o_ref[n, 0:block] * wide(mine, lat // 128) + carry[c, 0:block] * wide(theirs, lat // 128)

    for g in range(groups):
        weights[g].wait()
        if g == 0:
            wuk_copy.wait()
        project(hid_ref[...], cos_ref[...], sin_ref[...], g, store_own)
    for n in range(lat // 128):
        qs_v[:, n * 128:(n + 1) * 128] = qs_f[n].astype(BF16)
    qs_v[:, lat:lat + rope] = qs_f[lat // 128][:, 0:rope].astype(BF16)
    kv_copy.wait()
    kv_send.wait()
    outs = [pltpu.make_async_copy(qs_v, qs_hbm, out_sem.at[0])]
    own_targets, d_targets = [(6, own_v, 0), (7, own_v, 1)], [(4, diag, 0), (5, diag, 1)]
    plain, added = [(0, x_v, 0), (3, y_v, 1)], [(1, x_v, 1), (2, y_v, 0)]
    attend(own_targets, between=outs)
    close(own_targets)
    outs.append(pltpu.make_async_copy(own_v, own_hbm, out_sem.at[5]))

    for copy in gathers:
        copy.wait()
    hid3 = hid_all[...].reshape(3 * rows, hid_ref.shape[1])
    cos3 = jnp.concatenate([cos_all[p] for p in range(3)], axis=0)
    sin3 = jnp.concatenate([sin_all[p] for p in range(3)], axis=0)
    for g in range(groups):
        project(hid3, cos3, sin3, g, store_peer)

    attend(d_targets)
    close(d_targets)
    over = [remote(diag.at[0], carry.at[0], 10, to_x), remote(diag.at[1], carry.at[1], 11, to_y)]
    attend(plain, between=[*over, outs[1]])
    close(plain)
    early = [remote(x_v.at[0, 0:soon], soon_x_hbm, 12, to_x), remote(y_v.at[1, 0:soon], soon_y_hbm, 13, to_y)]
    outs.append(pltpu.make_async_copy(x_v.at[0, soon:block + TAIL], x_hbm.at[0:rest], out_sem.at[1]))
    outs.append(pltpu.make_async_copy(y_v.at[1, soon:block + TAIL], y_hbm.at[block + TAIL:rest + block + TAIL], out_sem.at[2]))
    attend(added, between=[*early, *outs[2:]])
    for copy in over:
        copy.wait()
    merge(1, x_v, 1, 1)
    merge(2, y_v, 0, 0)
    close(added)
    last = [pltpu.make_async_copy(x_v.at[1], x_hbm.at[rest:rest + block + TAIL], out_sem.at[3]),
            pltpu.make_async_copy(y_v.at[0], y_hbm.at[0:block + TAIL], out_sem.at[4])]
    for copy in last:
        copy.start()
    for copy in (*outs, *early, *last):
        copy.wait()


def prefix_phase(hidden, w_q, w_uk, kv_own, seq_lens, first_pos, log2_scale, chunk=1024, soon=32):
    rows, dim = hidden.shape
    n_head, nope, lat = w_uk.shape
    qk = w_q.shape[1] // n_head
    rope = qk - nope
    inv_freq = jnp.exp(jnp.arange(rope // 2, dtype=F32) * (-math.log(ROPE_BASE) / (rope // 2)))
    angle = (first_pos + seq_lens).astype(F32)[:, None] * inv_freq
    block = n_head // 2 * rows
    payload = jax.ShapeDtypeStruct((2, block + TAIL, lat), F32)
    early = jax.ShapeDtypeStruct((soon, lat), F32)
    later = jax.ShapeDtypeStruct((2 * (block + TAIL) - soon, lat), F32)
    in_hbm = pl.BlockSpec(memory_space=pltpu.HBM)
    return pl.pallas_call(
        functools.partial(prefix_kernel, n_head, nope, rope, log2_scale),
        out_shape=(jax.ShapeDtypeStruct((rows * n_head, lat + rope), BF16), payload, later, later, early, early),
        in_specs=[vmem(), vmem(), vmem(), in_hbm, in_hbm, in_hbm],
        out_specs=(in_hbm,) * 6,
        scratch_shapes=[
            pltpu.VMEM((3, rows, dim), BF16), pltpu.VMEM((3, rows, rope // 2), F32), pltpu.VMEM((3, rows, rope // 2), F32),
            pltpu.VMEM(w_q.shape, BF16), pltpu.VMEM(w_uk.shape, BF16), pltpu.VMEM((2, *kv_own.shape), BF16),
            pltpu.VMEM((8, block, lat + rope), BF16), pltpu.VMEM((lat // 128 + 1, rows * n_head, 128), F32),
            pltpu.VMEM((rows * n_head, lat + rope), BF16),
            pltpu.VMEM((8, block, 128), F32), pltpu.VMEM((8, block, 128), F32),
            pltpu.VMEM((4, block, chunk), F32), pltpu.VMEM((4, block, chunk), BF16),
            *[pltpu.VMEM(payload.shape, F32)] * 5,
            pltpu.SemaphoreType.DMA((n_head // 4,)), pltpu.SemaphoreType.DMA((2,)), pltpu.SemaphoreType.DMA((6,)),
            pltpu.SemaphoreType.DMA((14,)), pltpu.SemaphoreType.DMA((14,))],
        compiler_params=pltpu.CompilerParams(collective_id=0, has_side_effects=True, vmem_limit_bytes=60 * MIB),
        name='prefix',
    )(hidden, jnp.cos(angle), jnp.sin(angle), w_q, w_uk, kv_own)


def suffix_kernel(log2_scale, lat, chunk, unit, ring, streamed, lens_ref, q_hbm, kv_hbm, o_ref, m_ref, l_ref,
                  q_ref, kv_v, s_v, m_v, l_v, acc, sems, q_sem, b_s, c_s):
    n_seq = lens_ref.shape[0]
    heads = q_hbm.shape[0] // n_seq
    shift = chunk.bit_length() - 1
    q_copy = pltpu.make_async_copy(q_hbm, q_ref, q_sem)
    q_copy.start()
    total = jnp.int32(0)
    for b in range(n_seq):
        total += lax.shift_right_logical(lens_ref[b], shift) + 1
    trips = lax.div(total + unit - 1, unit)
    depth = ring - 2

    def start(at, group, live):
        b, c = at
        for u in range(unit):
            b_s[group * unit + u] = b
            c_s[group * unit + u] = c
            have = jnp.minimum(b, n_seq - 1)

            @pl.when(live)
            def _(u=u, c=c, have=have):
                pltpu.make_async_copy(
                    kv_hbm.at[have, :, pl.ds(pl.multiple_of(c * chunk, chunk), chunk)], kv_v.at[group, u], sems.at[group]).start()
            last = c >= lax.shift_right_logical(lens_ref[have], shift)
            b, c = jnp.where(last, jnp.minimum(b + 1, n_seq), b), jnp.where(last, 0, c + 1)
        return b, c

    for u in range(unit):
        b_s[(ring - 1) * unit + u] = n_seq
        c_s[(ring - 1) * unit + u] = 0
    ahead = lax.fori_loop(0, depth, lambda j, at: start(at, j, j < trips), (jnp.int32(0), jnp.int32(0)))

    def step(i, at):
        base, prev, far = [lax.rem(i + d, ring) for d in (0, ring - 1, depth)]

        @pl.when(i < trips)
        def _():
            pltpu.make_async_copy(kv_v.at[base], kv_v.at[base], sems.at[base]).wait()

        here, there = lax.rem(i, 2), lax.rem(i + 1, 2)
        for u in range(unit):
            bq = jnp.minimum(b_s[base * unit + u], n_seq - 1)
            q = q_ref[pl.ds(pl.multiple_of(bq * heads, heads), heads), :]
            s_v[here, u] = jnp.dot(q, kv_v[base, u], preferred_element_type=F32)

        lanes = lax.broadcasted_iota(jnp.int32, (heads, chunk), 1)
        items = [(b_s[prev * unit + u], c_s[prev * unit + u]) for u in range(unit)]
        scores = []
        for u, (b, c) in enumerate(items):
            length = lens_ref[jnp.minimum(b, n_seq - 1)]
            scores.append(jnp.where(lanes <= length - c * chunk, s_v[there, u], -jnp.inf))
        top = jnp.max(jnp.concatenate(scores, axis=0), axis=1, keepdims=True)
        m_old, l_old, o_old = m_v[...], l_v[...], acc[...]
        for u, (b, c) in enumerate(items):
            first = c == 0
            m_old = jnp.where(first, -jnp.inf, m_old)
            m_new = jnp.maximum(m_old, top[u * heads:(u + 1) * heads])
            alpha = jnp.exp2((m_old - m_new) * log2_scale)
            p = jnp.exp2((scores[u] - wide(m_new, chunk // 128)) * log2_scale)
            part = p[:, 0:128]
            for n in range(1, chunk // 128):
                part += p[:, n * 128:(n + 1) * 128]
            if u in streamed:
                added = jnp.transpose(lax.dot_general(kv_v[prev, u, 0:lat, :], p.astype(BF16), NT, preferred_element_type=F32))
            else:
                added = lax.dot_general(p.astype(BF16), kv_v[prev, u, 0:lat, :], NT, preferred_element_type=F32)
            l_old = jnp.where(first, 0.0, l_old * alpha) + part
            o_old = jnp.where(first, 0.0, o_old * wide(alpha, lat // 128)) + added
            m_old = m_new
            out = pl.ds(pl.multiple_of(b * heads, heads), heads)
            m_ref[out, :] = m_old
            l_ref[out, :] = l_old
            for n in range(lat // 128):
                o_ref[n, out, :] = o_old[:, n * 128:(n + 1) * 128]
        m_v[...], l_v[...], acc[...] = m_old, l_old, o_old
        return start(at, far, i + depth < trips)

    q_copy.wait()
    lax.fori_loop(0, trips + 1, step, ahead)


def suffix_part(q_seq, kv_suffix, seq_lens, log2_scale, lat, chunk=256, unit=8, ring=5, streamed=(1, 3, 5)):
    n_seq, slots, wide_row = kv_suffix.shape
    rows = q_seq.shape[0]
    heads = rows // n_seq
    flops = 2 * rows * slots * (wide_row + lat) * 4
    return pl.pallas_call(
        functools.partial(suffix_kernel, log2_scale, lat, chunk, unit, ring, streamed),
        out_shape=(jax.ShapeDtypeStruct((lat // 128, rows + heads, 128), F32), jax.ShapeDtypeStruct((rows + heads, 128), F32),
                   jax.ShapeDtypeStruct((rows + heads, 128), F32)),
        in_specs=[pl.BlockSpec(memory_space=pltpu.SMEM), hbm(), hbm()],
        out_specs=(vmem(), vmem(), vmem()),
        scratch_shapes=[pltpu.VMEM(q_seq.shape, BF16), pltpu.VMEM((ring, unit, wide_row, chunk), BF16), pltpu.VMEM((2, unit, heads, chunk), F32),
                        pltpu.VMEM((heads, 128), F32), pltpu.VMEM((heads, 128), F32),
                        pltpu.VMEM((heads, lat), F32), pltpu.SemaphoreType.DMA((ring,)), pltpu.SemaphoreType.DMA,
                        pltpu.SMEM((ring * unit,), jnp.int32), pltpu.SMEM((ring * unit,), jnp.int32)],
        compiler_params=pltpu.CompilerParams(vmem_limit_bytes=32 * MIB),
        cost_estimate=pl.CostEstimate(flops=flops, bytes_accessed=40 * MIB, transcendentals=0),
        name='suffix',
    )(seq_lens, q_seq, kv_suffix.swapaxes(1, 2))


def output_kernel(log2_scale, hid_ref, wuv_ref, wo_ref, so_ref, sm_ref, sl_ref, own_ref, x_ref, y_ref, soon_x_ref, soon_y_ref, out_ref):
    n_head = wuv_ref.shape[0]
    rows = hid_ref.shape[0]
    half = n_head // 2
    block = half * rows
    value = wuv_ref.shape[2]
    soon = soon_x_ref.shape[0]
    rest = block + TAIL - soon

    def sums_of(side, at):
        early = at < soon
        from_x = x_ref[rest + at:rest + at + rows] if side else soon_x_ref[at:at + rows] if early else x_ref[at - soon:at - soon + rows]
        low = block + TAIL + at - soon
        from_y = y_ref[at:at + rows] if not side else soon_y_ref[at:at + rows] if early else y_ref[low:low + rows]
        return own_ref[side, at:at + rows], from_x, from_y

    cols = []
    for side in range(2):
        x_low = rest + block if side else block - soon
        y_low = block + TAIL + block - soon if side else block
        for tail in (own_ref[side, block:block + TAIL], x_ref[x_low:x_low + TAIL], y_ref[y_low:y_low + TAIL]):
            cols.append((jnp.transpose(tail[:, 0:block])[:, 0:1], jnp.transpose(tail[:, block:2 * block])[:, 0:1]))
    out = hid_ref[...].astype(F32)
    values = []
    for h in range(n_head):
        side, at = h // half, (h % half) * rows
        mine = pl.ds(h, rows, stride=n_head)
        own = jnp.concatenate([so_ref[n, mine, :] for n in range(so_ref.shape[0])], axis=1)
        terms = [(own, sm_ref[mine, :][:, 0:1], jnp.sum(sl_ref[mine, :], axis=1, keepdims=True))]
        for k, o_part in enumerate(sums_of(side, at)):
            m_part, l_part = cols[side * 3 + k]
            terms.append((o_part, m_part[at:at + rows], l_part[at:at + rows]))
        m_all = functools.reduce(jnp.maximum, [t[1] for t in terms])
        o_sum, l_sum = 0.0, 0.0
        for o_part, m_part, l_part in terms:
            weight = jnp.exp2((m_part - m_all) * log2_scale)
            o_sum += o_part * weight
            l_sum += l_part * weight
        o_lat = (o_sum / l_sum).astype(BF16)
        values.append(jnp.dot(o_lat, wuv_ref[h], preferred_element_type=F32).astype(BF16))
        if len(values) == 4:
            low = (h - 3) * value
            out += jnp.dot(jnp.concatenate(values, axis=1), wo_ref[low:low + 4 * value], preferred_element_type=F32)
            values = []
    out_ref[...] = out.astype(BF16)


def finish_output(hidden, w_uv, w_o, suffix, parts, log2_scale):
    return pl.pallas_call(
        functools.partial(output_kernel, log2_scale),
        out_shape=jax.ShapeDtypeStruct(hidden.shape, BF16),
        in_specs=[vmem()] * 11,
        out_specs=vmem(),
        compiler_params=pltpu.CompilerParams(vmem_limit_bytes=32 * MIB),
        name='output',
    )(hidden, w_uv, w_o, *suffix, *parts)


def solution(mesh):
    group = mesh.shape['ctx']
    rows_spec = P(('dp', 'ctx'), None)
    whole_spec = P()
    over_x = [(i, i ^ 2) for i in range(group)]
    over_y = [(i, i ^ 4) for i in range(group)]

    def local_step(hidden, w_q, w_uk, w_uv, w_o, kv_prefix, kv_suffix, seq_lens):
        lat = w_uk.shape[2]
        n_head = w_uk.shape[0]
        log2_scale = LOG2E * (w_q.shape[1] // n_head) ** -0.5
        kv_own = kv_prefix.swapaxes(0, 1)
        q_seq, own, to_x, to_y, soon_x, soon_y = prefix_phase(hidden, w_q, w_uk, kv_own, seq_lens, kv_prefix.shape[0] * group, log2_scale)
        got_x, got_y = lax.ppermute(to_x, 'ctx', over_x), lax.ppermute(to_y, 'ctx', over_y)
        suffix = suffix_part(q_seq, kv_suffix, seq_lens, log2_scale, lat)
        return finish_output(hidden, w_uv, w_o, suffix, (own, got_x, got_y, soon_x, soon_y), log2_scale)

    return jax.shard_map(local_step, mesh=mesh, in_specs=(rows_spec, whole_spec, whole_spec, whole_spec, whole_spec, rows_spec, P(('dp', 'ctx'), None, None), P(('dp', 'ctx'))), out_specs=rows_spec, check_vma=False)
```

```python
import functools
import math
import jax
import jax.numpy as jnp
from jax import lax
from jax.experimental import pallas as pl
from jax.experimental.pallas import tpu as pltpu
from jax.sharding import PartitionSpec as P

ROPE_BASE = 10000
LOG2E = 1.4426950408889634
NT = (((1,), (1,)), ((), ()))
F32 = jnp.float32
BF16 = jnp.bfloat16
MIB = 1024 * 1024
TAIL = 8


def vmem():
    return pl.BlockSpec(memory_space=pltpu.VMEM)


def hbm():
    return pl.BlockSpec(memory_space=pl.ANY)


def wide(x, n):
    return jnp.concatenate([x] * n, axis=1)


def prefix_kernel(n_head, nope, rope, log2_scale, first_pos, lens_ref, hid_ref, freq_ref, wq_hbm, wuk_hbm, kv_hbm,
                  qs_hbm, own_hbm, x_hbm, y_hbm, soon_x_hbm, soon_y_hbm,
                  cos_ref, sin_ref, hid_all, cos_all, sin_all, wq_v, wuk_v, kv_v, q_v, qs_f, qs_v, m_v, l_v, s_v, p_v,
                  own_v, x_v, y_v, diag, carry, wq_sem, own_sem, out_sem, send_sem, recv_sem):
    rows = hid_ref.shape[0]
    lat = wuk_v.shape[2]
    qk = nope + rope
    per = 4
    groups = n_head // per
    width = per * qk
    half = n_head // 2
    block = half * rows
    chunk = s_v.shape[2]
    soon = soon_x_hbm.shape[0]
    rest = block + TAIL - soon
    me = lax.axis_index('ctx')
    core = lax.rem(me, 2)
    xx = lax.rem(me // 2, 2)
    yy = me // 4
    sib = me + 1 - 2 * core
    to_x = me + 2 - 4 * xx
    to_y = me + 4 - 8 * yy
    to_d = me + 6 - 4 * xx - 8 * yy
    weights = []
    for g in range(groups):
        cols = pl.ds(g * width, width)
        weights.append(pltpu.make_async_copy(wq_hbm.at[:, cols], wq_v.at[:, cols], wq_sem.at[g]))
    wuk_copy = pltpu.make_async_copy(wuk_hbm, wuk_v, own_sem.at[0])
    kv_copy = pltpu.make_async_copy(kv_hbm, kv_v.at[0], own_sem.at[1])
    for copy in (weights[0], wuk_copy, *weights[1:], kv_copy):
        copy.start()

    row = lax.broadcasted_iota(jnp.int32, cos_ref.shape, 0)
    pos = jnp.zeros(cos_ref.shape, jnp.int32)
    for b in range(rows):
        pos = jnp.where(row == b, first_pos + lens_ref[b], pos)
    angle = pos.astype(F32) * freq_ref[...]
    cos_ref[...] = jnp.cos(angle)
    sin_ref[...] = jnp.sin(angle)

    barrier = pltpu.get_barrier_semaphore()
    for peer in (sib, to_x, to_y, to_d):
        pl.semaphore_signal(barrier, inc=1, device_id={'ctx': peer})
    pl.semaphore_wait(barrier, 4)

    def remote(src, dst, n, peer):
        return pltpu.make_async_remote_copy(
            src_ref=src, dst_ref=dst, send_sem=send_sem.at[n], recv_sem=recv_sem.at[n], device_id={'ctx': peer})

    gathers = []
    for slot, peer in ((2, to_d), (0, to_x), (1, to_y)):
        gathers.append(remote(hid_ref, hid_all.at[slot], slot, peer))
        gathers.append(remote(cos_ref, cos_all.at[slot], 3 + slot, peer))
        gathers.append(remote(sin_ref, sin_all.at[slot], 6 + slot, peer))
    kv_send = remote(kv_hbm, kv_v.at[1], 9, sib)
    for copy in (*gathers, kv_send):
        copy.start()

    i = lax.broadcasted_iota(jnp.int32, (rope, rope), 0)
    j = lax.broadcasted_iota(jnp.int32, (rope, rope), 1)
    rot = jnp.where(i == j + rope // 2, -1.0, jnp.where(i + rope // 2 == j, 1.0, 0.0)).astype(BF16)

    def project(hid, cos, sin, g, store):
        q_all = jnp.dot(hid, wq_v[:, g * width:(g + 1) * width], preferred_element_type=F32)
        for n in range(per):
            q_nope = q_all[:, n * qk:n * qk + nope].astype(BF16)
            q_pe = q_all[:, n * qk + nope:(n + 1) * qk].astype(BF16)
            q_lat = jnp.dot(q_nope, wuk_v[g * per + n], preferred_element_type=F32).astype(BF16)
            turned = jnp.dot(q_pe, rot, preferred_element_type=F32)
            q_rot = (q_pe.astype(F32) * wide(cos, 2) + turned * wide(sin, 2)).astype(BF16)
            store(g * per + n, q_lat, q_rot)

    def keep(peer, h, q_lat, q_rot):
        at = slice((h % half) * rows, (h % half + 1) * rows)
        q_v[2 * peer + h // half, at, 0:lat] = q_lat
        q_v[2 * peer + h // half, at, lat:lat + rope] = q_rot

    def store_own(h, q_lat, q_rot):
        keep(3, h, q_lat, q_rot)
        for n in range(lat // 128):
            qs_f[n, pl.ds(h, rows, stride=n_head), :] = q_lat[:, n * 128:(n + 1) * 128].astype(F32)
        qs_f[lat // 128, pl.ds(h, rows, stride=n_head), :] = wide(q_rot, 2).astype(F32)

    def store_peer(h, q_lat, q_rot):
        for p in range(3):
            keep(p, h, q_lat[p * rows:(p + 1) * rows], q_rot[p * rows:(p + 1) * rows])

    def attend(targets, between=()):
        for b, o_ref, n in targets:
            o_ref[n, 0:block] = jnp.zeros((block, lat), F32)
            m_v[b] = jnp.full((block, 128), -jnp.inf, F32)
            l_v[b] = jnp.zeros((block, 128), F32)
        for copy in between:
            copy.start()

        def visit(i, _):
            keys = pl.ds(pl.multiple_of(i * chunk, chunk), chunk)
            items = [(k, *target) for k in range(2) for target in targets]
            def score(t):
                k, b = items[t][:2]
                s_v[t] = jnp.dot(q_v[b], kv_v[k, :, keys], preferred_element_type=F32)

            score(0)
            for t, (k, b, o_ref, n) in enumerate(items):
                if t + 1 < len(items):
                    score(t + 1)
                for r in range(0, block, 64):
                    at = slice(r, r + 64)
                    s = s_v[t, at]
                    m_old = m_v[b, at]
                    m_new = jnp.maximum(m_old, jnp.max(s, axis=1, keepdims=True))
                    alpha = jnp.exp2((m_old - m_new) * log2_scale)
                    p = jnp.exp2((s - wide(m_new, chunk // 128)) * log2_scale)
                    part = p[:, 0:128]
                    for c in range(1, chunk // 128):
                        part += p[:, c * 128:(c + 1) * 128]
                    l_v[b, at] = l_v[b, at] * alpha + part
                    m_v[b, at] = m_new
                    p_v[t, at] = p.astype(BF16)
                    o_ref[n, at] = o_ref[n, at] * wide(alpha, lat // 128)
                o_ref[n, 0:block] += lax.dot_general(p_v[t], kv_v[k, 0:lat, keys], NT, preferred_element_type=F32)
            return 0

        lax.fori_loop(0, kv_v.shape[2] // chunk, visit, 0)

    def close(targets):
        for b, o_ref, n in targets:
            o_ref[n, block:block + TAIL, 0:block] = jnp.transpose(m_v[b])[0:TAIL]
            l_sum = jnp.broadcast_to(jnp.sum(l_v[b], axis=1, keepdims=True), (block, 128))
            o_ref[n, block:block + TAIL, block:2 * block] = jnp.transpose(l_sum)[0:TAIL]

    def merge(b, o_ref, n, c):
        m_in = jnp.broadcast_to(jnp.transpose(carry[c, block:block + TAIL, 0:block])[:, 0:1], (block, 128))
        l_in = jnp.transpose(carry[c, block:block + TAIL, block:2 * block])[:, 0:1]
        m_new = jnp.maximum(m_v[b], m_in)
        mine = jnp.exp2((m_v[b] - m_new) * log2_scale)
        theirs = jnp.exp2((m_in - m_new) * log2_scale)
        first_lane = lax.broadcasted_iota(jnp.int32, (block, 128), 1) == 0
        l_v[b] = l_v[b] * mine + jnp.where(first_lane, l_in * theirs, 0.0)
        m_v[b] = m_new
        o_ref[n, 0:block] = o_ref[n, 0:block] * wide(mine, lat // 128) + carry[c, 0:block] * wide(theirs, lat // 128)

    for g in range(groups):
        weights[g].wait()
        if g == 0:
            wuk_copy.wait()
        project(hid_ref[...], cos_ref[...], sin_ref[...], g, store_own)
    for n in range(lat // 128):
        qs_v[:, n * 128:(n + 1) * 128] = qs_f[n].astype(BF16)
    qs_v[:, lat:lat + rope] = qs_f[lat // 128][:, 0:rope].astype(BF16)
    kv_copy.wait()
    kv_send.wait()
    outs = [pltpu.make_async_copy(qs_v, qs_hbm.at[0], out_sem.at[0])]
    own_targets, d_targets = [(6, own_v, 0), (7, own_v, 1)], [(4, diag, 0), (5, diag, 1)]
    plain, added = [(0, x_v, 0), (3, y_v, 1)], [(1, x_v, 1), (2, y_v, 0)]
    attend(own_targets[:1], between=outs)

    for copy in gathers:
        copy.wait()
    hid3 = hid_all[...].reshape(3 * rows, hid_ref.shape[1])
    cos3 = jnp.concatenate([cos_all[p] for p in range(3)], axis=0)
    sin3 = jnp.concatenate([sin_all[p] for p in range(3)], axis=0)
    for g in range(groups):
        project(hid3, cos3, sin3, g, store_peer)

    attend(d_targets)
    close(d_targets)
    over = [remote(diag.at[0], carry.at[0], 10, to_x), remote(diag.at[1], carry.at[1], 11, to_y)]
    attend(own_targets[1:], between=over)
    close(own_targets)
    outs.append(pltpu.make_async_copy(own_v, own_hbm, out_sem.at[5]))
    attend(plain, between=outs[1:])
    close(plain)
    early = [remote(x_v.at[0, 0:soon], soon_x_hbm, 12, to_x), remote(y_v.at[1, 0:soon], soon_y_hbm, 13, to_y)]
    outs.append(pltpu.make_async_copy(x_v.at[0, soon:block + TAIL], x_hbm.at[0:rest], out_sem.at[1]))
    outs.append(pltpu.make_async_copy(y_v.at[1, soon:block + TAIL], y_hbm.at[block + TAIL:rest + block + TAIL], out_sem.at[2]))
    attend(added, between=[*early, *outs[2:]])
    for copy in over:
        copy.wait()
    merge(1, x_v, 1, 1)
    merge(2, y_v, 0, 0)
    close(added)
    last = [pltpu.make_async_copy(x_v.at[1], x_hbm.at[rest:rest + block + TAIL], out_sem.at[3]),
            pltpu.make_async_copy(y_v.at[0], y_hbm.at[0:block + TAIL], out_sem.at[4])]
    for copy in last:
        copy.start()
    for copy in (*outs, *early, *last):
        copy.wait()


def prefix_phase(hidden, w_q, w_uk, kv_own, seq_lens, first_pos, log2_scale, chunk=1024, soon=96):
    rows, dim = hidden.shape
    n_head, nope, lat = w_uk.shape
    qk = w_q.shape[1] // n_head
    rope = qk - nope
    inv_freq = jnp.exp(jnp.arange(rope // 2, dtype=F32) * (-math.log(ROPE_BASE) / (rope // 2)))[None, :]
    block = n_head // 2 * rows
    payload = jax.ShapeDtypeStruct((2, block + TAIL, lat), F32)
    early = jax.ShapeDtypeStruct((soon, lat), F32)
    later = jax.ShapeDtypeStruct((2 * (block + TAIL) - soon, lat), F32)
    in_hbm = pl.BlockSpec(memory_space=pltpu.HBM)
    return pl.pallas_call(
        functools.partial(prefix_kernel, n_head, nope, rope, log2_scale, first_pos),
        out_shape=(jax.ShapeDtypeStruct((64, rows * n_head, lat + rope), BF16), payload, later, later, early, early),
        in_specs=[pl.BlockSpec(memory_space=pltpu.SMEM), vmem(), vmem(), in_hbm, in_hbm, in_hbm],
        out_specs=(in_hbm,) * 6,
        scratch_shapes=[
            pltpu.VMEM((rows, rope // 2), F32), pltpu.VMEM((rows, rope // 2), F32),
            pltpu.VMEM((3, rows, dim), BF16), pltpu.VMEM((3, rows, rope // 2), F32), pltpu.VMEM((3, rows, rope // 2), F32),
            pltpu.VMEM(w_q.shape, BF16), pltpu.VMEM(w_uk.shape, BF16), pltpu.VMEM((2, *kv_own.shape), BF16),
            pltpu.VMEM((8, block, lat + rope), BF16), pltpu.VMEM((lat // 128 + 1, rows * n_head, 128), F32),
            pltpu.VMEM((rows * n_head, lat + rope), BF16),
            pltpu.VMEM((8, block, 128), F32), pltpu.VMEM((8, block, 128), F32),
            pltpu.VMEM((4, block, chunk), F32), pltpu.VMEM((4, block, chunk), BF16),
            *[pltpu.VMEM(payload.shape, F32)] * 5,
            pltpu.SemaphoreType.DMA((n_head // 4,)), pltpu.SemaphoreType.DMA((2,)), pltpu.SemaphoreType.DMA((6,)),
            pltpu.SemaphoreType.DMA((14,)), pltpu.SemaphoreType.DMA((14,))],
        compiler_params=pltpu.CompilerParams(collective_id=0, has_side_effects=True, vmem_limit_bytes=60 * MIB),
        name='prefix',
    )(seq_lens, hidden, inv_freq, w_q, w_uk, kv_own)


def suffix_kernel(log2_scale, lat, chunk, unit, ring, streamed, lens_ref, q_hbm, kv_hbm, o_ref, m_ref, l_ref,
                  q_ref, kv_v, s_v, m_v, l_v, acc, sems, q_sem, b_s, c_s):
    n_seq = lens_ref.shape[0]
    heads = q_hbm.shape[1] // n_seq
    shift = chunk.bit_length() - 1
    q_copy = pltpu.make_async_copy(q_hbm.at[0], q_ref, q_sem)
    q_copy.start()
    total = jnp.int32(0)
    for b in range(n_seq):
        total += lax.shift_right_logical(lens_ref[b], shift) + 1
    trips = lax.div(total + unit - 1, unit)
    depth = ring - 2

    def start(at, group, live):
        b, c = at
        for u in range(unit):
            b_s[group * unit + u] = b
            c_s[group * unit + u] = c
            have = jnp.minimum(b, n_seq - 1)

            @pl.when(live)
            def _(u=u, c=c, have=have):
                pltpu.make_async_copy(
                    kv_hbm.at[have, :, pl.ds(pl.multiple_of(c * chunk, chunk), chunk)], kv_v.at[group, u], sems.at[group]).start()
            last = c >= lax.shift_right_logical(lens_ref[have], shift)
            b, c = jnp.where(last, jnp.minimum(b + 1, n_seq), b), jnp.where(last, 0, c + 1)
        return b, c

    for u in range(unit):
        b_s[(ring - 1) * unit + u] = n_seq
        c_s[(ring - 1) * unit + u] = 0
    ahead = lax.fori_loop(0, depth, lambda j, at: start(at, j, j < trips), (jnp.int32(0), jnp.int32(0)))

    def step(i, at):
        base, prev, far = [lax.rem(i + d, ring) for d in (0, ring - 1, depth)]

        @pl.when(i < trips)
        def _():
            pltpu.make_async_copy(kv_v.at[base], kv_v.at[base], sems.at[base]).wait()

        here, there = lax.rem(i, 2), lax.rem(i + 1, 2)
        for u in range(unit):
            bq = jnp.minimum(b_s[base * unit + u], n_seq - 1)
            q = q_ref[pl.ds(pl.multiple_of(bq * heads, heads), heads), :]
            s_v[here, u] = jnp.dot(q, kv_v[base, u], preferred_element_type=F32)

        lanes = lax.broadcasted_iota(jnp.int32, (heads, chunk), 1)
        items = [(b_s[prev * unit + u], c_s[prev * unit + u]) for u in range(unit)]
        scores = []
        for u, (b, c) in enumerate(items):
            length = lens_ref[jnp.minimum(b, n_seq - 1)]
            scores.append(jnp.where(lanes <= length - c * chunk, s_v[there, u], -jnp.inf))
        top = jnp.max(jnp.concatenate(scores, axis=0), axis=1, keepdims=True)
        m_old, l_old, o_old = m_v[...], l_v[...], acc[...]
        for u, (b, c) in enumerate(items):
            first = c == 0
            m_old = jnp.where(first, -jnp.inf, m_old)
            m_new = jnp.maximum(m_old, top[u * heads:(u + 1) * heads])
            alpha = jnp.exp2((m_old - m_new) * log2_scale)
            p = jnp.exp2((scores[u] - wide(m_new, chunk // 128)) * log2_scale)
            part = p[:, 0:128]
            for n in range(1, chunk // 128):
                part += p[:, n * 128:(n + 1) * 128]
            if u in streamed:
                added = jnp.transpose(lax.dot_general(kv_v[prev, u, 0:lat, :], p.astype(BF16), NT, preferred_element_type=F32))
            else:
                added = lax.dot_general(p.astype(BF16), kv_v[prev, u, 0:lat, :], NT, preferred_element_type=F32)
            l_old = jnp.where(first, 0.0, l_old * alpha) + part
            o_old = jnp.where(first, 0.0, o_old * wide(alpha, lat // 128)) + added
            m_old = m_new
            out = pl.ds(pl.multiple_of(b * heads, heads), heads)
            m_ref[out, :] = m_old
            l_ref[out, :] = l_old
            for n in range(lat // 128):
                o_ref[n, out, :] = o_old[:, n * 128:(n + 1) * 128]
        m_v[...], l_v[...], acc[...] = m_old, l_old, o_old
        return start(at, far, i + depth < trips)

    q_copy.wait()
    lax.fori_loop(0, trips + 1, step, ahead)


def suffix_part(q_seq, kv_suffix, seq_lens, log2_scale, lat, chunk=256, unit=8, ring=5, streamed=(1, 3, 5)):
    n_seq, slots, wide_row = kv_suffix.shape
    rows = q_seq.shape[1]
    heads = rows // n_seq
    flops = 2 * rows * slots * (wide_row + lat) * 4
    return pl.pallas_call(
        functools.partial(suffix_kernel, log2_scale, lat, chunk, unit, ring, streamed),
        out_shape=(jax.ShapeDtypeStruct((lat // 128, rows + heads, 128), F32), jax.ShapeDtypeStruct((rows + heads, 128), F32),
                   jax.ShapeDtypeStruct((rows + heads, 128), F32)),
        in_specs=[pl.BlockSpec(memory_space=pltpu.SMEM), hbm(), hbm()],
        out_specs=(vmem(), vmem(), vmem()),
        scratch_shapes=[pltpu.VMEM(q_seq.shape[1:], BF16), pltpu.VMEM((ring, unit, wide_row, chunk), BF16), pltpu.VMEM((2, unit, heads, chunk), F32),
                        pltpu.VMEM((heads, 128), F32), pltpu.VMEM((heads, 128), F32),
                        pltpu.VMEM((heads, lat), F32), pltpu.SemaphoreType.DMA((ring,)), pltpu.SemaphoreType.DMA,
                        pltpu.SMEM((ring * unit,), jnp.int32), pltpu.SMEM((ring * unit,), jnp.int32)],
        compiler_params=pltpu.CompilerParams(vmem_limit_bytes=32 * MIB),
        cost_estimate=pl.CostEstimate(flops=flops, bytes_accessed=40 * MIB, transcendentals=0),
        name='suffix',
    )(seq_lens, q_seq, kv_suffix.swapaxes(1, 2))


def output_kernel(log2_scale, hid_ref, wuv_ref, wo_ref, so_ref, sm_ref, sl_ref, own_ref, x_ref, y_ref, soon_x_ref, soon_y_ref, out_ref):
    n_head = wuv_ref.shape[0]
    rows = hid_ref.shape[0]
    half = n_head // 2
    block = half * rows
    value = wuv_ref.shape[2]
    soon = soon_x_ref.shape[0]
    rest = block + TAIL - soon

    def sums_of(side, at):
        early = at < soon
        from_x = x_ref[rest + at:rest + at + rows] if side else soon_x_ref[at:at + rows] if early else x_ref[at - soon:at - soon + rows]
        low = block + TAIL + at - soon
        from_y = y_ref[at:at + rows] if not side else soon_y_ref[at:at + rows] if early else y_ref[low:low + rows]
        return own_ref[side, at:at + rows], from_x, from_y

    cols = []
    for side in range(2):
        x_low = rest + block if side else block - soon
        y_low = block + TAIL + block - soon if side else block
        for tail in (own_ref[side, block:block + TAIL], x_ref[x_low:x_low + TAIL], y_ref[y_low:y_low + TAIL]):
            cols.append((jnp.transpose(tail[:, 0:block])[:, 0:1], jnp.transpose(tail[:, block:2 * block])[:, 0:1]))
    out = hid_ref[...].astype(F32)
    values = []
    for h in range(n_head):
        side, at = h // half, (h % half) * rows
        mine = pl.ds(h, rows, stride=n_head)
        own = jnp.concatenate([so_ref[n, mine, :] for n in range(so_ref.shape[0])], axis=1)
        terms = [(own, sm_ref[mine, :][:, 0:1], jnp.sum(sl_ref[mine, :], axis=1, keepdims=True))]
        for k, o_part in enumerate(sums_of(side, at)):
            m_part, l_part = cols[side * 3 + k]
            terms.append((o_part, m_part[at:at + rows], l_part[at:at + rows]))
        m_all = functools.reduce(jnp.maximum, [t[1] for t in terms])
        o_sum, l_sum = 0.0, 0.0
        for o_part, m_part, l_part in terms:
            weight = jnp.exp2((m_part - m_all) * log2_scale)
            o_sum += o_part * weight
            l_sum += l_part * weight
        o_lat = (o_sum / l_sum).astype(BF16)
        values.append(jnp.dot(o_lat, wuv_ref[h], preferred_element_type=F32).astype(BF16))
        if len(values) == 4:
            low = (h - 3) * value
            out += jnp.dot(jnp.concatenate(values, axis=1), wo_ref[low:low + 4 * value], preferred_element_type=F32)
            values = []
    out_ref[...] = out.astype(BF16)


def finish_output(hidden, w_uv, w_o, suffix, parts, log2_scale):
    return pl.pallas_call(
        functools.partial(output_kernel, log2_scale),
        out_shape=jax.ShapeDtypeStruct(hidden.shape, BF16),
        in_specs=[vmem()] * 11,
        out_specs=vmem(),
        compiler_params=pltpu.CompilerParams(vmem_limit_bytes=32 * MIB),
        name='output',
    )(hidden, w_uv, w_o, *suffix, *parts)


def solution(mesh):
    group = mesh.shape['ctx']
    rows_spec = P(('dp', 'ctx'), None)
    whole_spec = P()
    over_x = [(i, i ^ 2) for i in range(group)]
    over_y = [(i, i ^ 4) for i in range(group)]

    def local_step(hidden, w_q, w_uk, w_uv, w_o, kv_prefix, kv_suffix, seq_lens):
        lat = w_uk.shape[2]
        n_head = w_uk.shape[0]
        log2_scale = LOG2E * (w_q.shape[1] // n_head) ** -0.5
        kv_own = kv_prefix.swapaxes(0, 1)
        q_seq, own, to_x, to_y, soon_x, soon_y = prefix_phase(hidden, w_q, w_uk, kv_own, seq_lens, kv_prefix.shape[0] * group, log2_scale)
        got_x, got_y = lax.ppermute(to_x, 'ctx', over_x), lax.ppermute(to_y, 'ctx', over_y)
        suffix = suffix_part(q_seq, kv_suffix, seq_lens, log2_scale, lat)
        return finish_output(hidden, w_uv, w_o, suffix, (own, got_x, got_y, soon_x, soon_y), log2_scale)

    return jax.shard_map(local_step, mesh=mesh, in_specs=(rows_spec, whole_spec, whole_spec, whole_spec, whole_spec, rows_spec, P(('dp', 'ctx'), None, None), P(('dp', 'ctx'))), out_specs=rows_spec, check_vma=False)
```

```python
import functools
import math
import jax
import jax.numpy as jnp
from jax import lax
from jax.experimental import pallas as pl
from jax.experimental.pallas import tpu as pltpu
from jax.sharding import PartitionSpec as P

ROPE_BASE = 10000
LOG2E = 1.4426950408889634
NT = (((1,), (1,)), ((), ()))
F32 = jnp.float32
BF16 = jnp.bfloat16
MIB = 1024 * 1024
TAIL = 8


def vmem():
    return pl.BlockSpec(memory_space=pltpu.VMEM)


def hbm():
    return pl.BlockSpec(memory_space=pl.ANY)


def wide(x, n):
    return jnp.concatenate([x] * n, axis=1)


def prefix_kernel(n_head, nope, rope, log2_scale, first_pos, lens_ref, hid_hbm, freq_ref, wq_hbm, wuk_hbm, kv_hbm,
                  qs_hbm, own_hbm, x_hbm, y_hbm, soon_x_hbm, soon_y_hbm,
                  hid_ref, cos_ref, sin_ref, hid_all, cos_all, sin_all, wq_v, wuk_v, kv_v, q_v, qs_f, qs_v, m_v, l_v, s_v, p_v,
                  own_v, x_v, y_v, diag, carry, wq_sem, own_sem, out_sem, send_sem, recv_sem):
    rows = hid_ref.shape[0]
    lat = wuk_v.shape[2]
    qk = nope + rope
    per = 4
    groups = n_head // per
    width = per * qk
    half = n_head // 2
    block = half * rows
    chunk = s_v.shape[2]
    soon = soon_x_hbm.shape[0]
    rest = block + TAIL - soon
    me = lax.axis_index('ctx')
    core = lax.rem(me, 2)
    xx = lax.rem(me // 2, 2)
    yy = me // 4
    sib = me + 1 - 2 * core
    to_x = me + 2 - 4 * xx
    to_y = me + 4 - 8 * yy
    to_d = me + 6 - 4 * xx - 8 * yy
    weights = []
    for g in range(groups):
        cols = pl.ds(g * width, width)
        weights.append(pltpu.make_async_copy(wq_hbm.at[:, cols], wq_v.at[:, cols], wq_sem.at[g]))
    wuk_copy = pltpu.make_async_copy(wuk_hbm, wuk_v, own_sem.at[0])
    kv_copy = pltpu.make_async_copy(kv_hbm, kv_v.at[0], own_sem.at[1])
    hid_copy = pltpu.make_async_copy(hid_hbm, hid_ref, own_sem.at[2])
    for copy in (hid_copy, weights[0], wuk_copy, *weights[1:], kv_copy):
        copy.start()

    row = lax.broadcasted_iota(jnp.int32, cos_ref.shape, 0)
    pos = jnp.zeros(cos_ref.shape, jnp.int32)
    for b in range(rows):
        pos = jnp.where(row == b, first_pos + lens_ref[b], pos)
    angle = pos.astype(F32) * freq_ref[...]
    cos_ref[...] = jnp.cos(angle)
    sin_ref[...] = jnp.sin(angle)

    barrier = pltpu.get_barrier_semaphore()
    for peer in (sib, to_x, to_y, to_d):
        pl.semaphore_signal(barrier, inc=1, device_id={'ctx': peer})
    pl.semaphore_wait(barrier, 4)
    hid_copy.wait()

    def remote(src, dst, n, peer):
        return pltpu.make_async_remote_copy(
            src_ref=src, dst_ref=dst, send_sem=send_sem.at[n], recv_sem=recv_sem.at[n], device_id={'ctx': peer})

    gathers = []
    for slot, peer in ((2, to_d), (0, to_x), (1, to_y)):
        gathers.append(remote(hid_ref, hid_all.at[slot], slot, peer))
        gathers.append(remote(cos_ref, cos_all.at[slot], 3 + slot, peer))
        gathers.append(remote(sin_ref, sin_all.at[slot], 6 + slot, peer))
    kv_send = remote(kv_hbm, kv_v.at[1], 9, sib)
    for copy in (*gathers, kv_send):
        copy.start()

    i = lax.broadcasted_iota(jnp.int32, (rope, rope), 0)
    j = lax.broadcasted_iota(jnp.int32, (rope, rope), 1)
    rot = jnp.where(i == j + rope // 2, -1.0, jnp.where(i + rope // 2 == j, 1.0, 0.0)).astype(BF16)

    def project(hid, cos, sin, g, store):
        q_all = jnp.dot(hid, wq_v[:, g * width:(g + 1) * width], preferred_element_type=F32)
        for n in range(per):
            q_nope = q_all[:, n * qk:n * qk + nope].astype(BF16)
            q_pe = q_all[:, n * qk + nope:(n + 1) * qk].astype(BF16)
            q_lat = jnp.dot(q_nope, wuk_v[g * per + n], preferred_element_type=F32).astype(BF16)
            turned = jnp.dot(q_pe, rot, preferred_element_type=F32)
            q_rot = (q_pe.astype(F32) * wide(cos, 2) + turned * wide(sin, 2)).astype(BF16)
            store(g * per + n, q_lat, q_rot)

    def keep(peer, h, q_lat, q_rot):
        at = slice((h % half) * rows, (h % half + 1) * rows)
        q_v[2 * peer + h // half, at, 0:lat] = q_lat
        q_v[2 * peer + h // half, at, lat:lat + rope] = q_rot

    def store_own(h, q_lat, q_rot):
        keep(3, h, q_lat, q_rot)
        for n in range(lat // 128):
            qs_f[n, pl.ds(h, rows, stride=n_head), :] = q_lat[:, n * 128:(n + 1) * 128].astype(F32)
        qs_f[lat // 128, pl.ds(h, rows, stride=n_head), :] = wide(q_rot, 2).astype(F32)

    def store_peer(h, q_lat, q_rot):
        for p in range(3):
            keep(p, h, q_lat[p * rows:(p + 1) * rows], q_rot[p * rows:(p + 1) * rows])

    def attend(targets, between=()):
        for b, o_ref, n in targets:
            o_ref[n, 0:block] = jnp.zeros((block, lat), F32)
            m_v[b] = jnp.full((block, 128), -jnp.inf, F32)
            l_v[b] = jnp.zeros((block, 128), F32)
        for copy in between:
            copy.start()

        def visit(i, _):
            keys = pl.ds(pl.multiple_of(i * chunk, chunk), chunk)
            items = [(k, *target) for k in range(2) for target in targets]
            def score(t):
                k, b = items[t][:2]
                s_v[t] = jnp.dot(q_v[b], kv_v[k, :, keys], preferred_element_type=F32)

            score(0)
            for t, (k, b, o_ref, n) in enumerate(items):
                if t + 1 < len(items):
                    score(t + 1)
                for r in range(0, block, 64):
                    at = slice(r, r + 64)
                    s = s_v[t, at]
                    m_old = m_v[b, at]
                    m_new = jnp.maximum(m_old, jnp.max(s, axis=1, keepdims=True))
                    alpha = jnp.exp2((m_old - m_new) * log2_scale)
                    p = jnp.exp2((s - wide(m_new, chunk // 128)) * log2_scale)
                    part = p[:, 0:128]
                    for c in range(1, chunk // 128):
                        part += p[:, c * 128:(c + 1) * 128]
                    l_v[b, at] = l_v[b, at] * alpha + part
                    m_v[b, at] = m_new
                    p_v[t, at] = p.astype(BF16)
                    o_ref[n, at] = o_ref[n, at] * wide(alpha, lat // 128)
                o_ref[n, 0:block] += lax.dot_general(p_v[t], kv_v[k, 0:lat, keys], NT, preferred_element_type=F32)
            return 0

        lax.fori_loop(0, kv_v.shape[2] // chunk, visit, 0)

    def close(targets):
        for b, o_ref, n in targets:
            o_ref[n, block:block + TAIL, 0:block] = jnp.transpose(m_v[b])[0:TAIL]
            l_sum = jnp.broadcast_to(jnp.sum(l_v[b], axis=1, keepdims=True), (block, 128))
            o_ref[n, block:block + TAIL, block:2 * block] = jnp.transpose(l_sum)[0:TAIL]

    def merge(b, o_ref, n, c):
        m_in = jnp.broadcast_to(jnp.transpose(carry[c, block:block + TAIL, 0:block])[:, 0:1], (block, 128))
        l_in = jnp.transpose(carry[c, block:block + TAIL, block:2 * block])[:, 0:1]
        m_new = jnp.maximum(m_v[b], m_in)
        mine = jnp.exp2((m_v[b] - m_new) * log2_scale)
        theirs = jnp.exp2((m_in - m_new) * log2_scale)
        first_lane = lax.broadcasted_iota(jnp.int32, (block, 128), 1) == 0
        l_v[b] = l_v[b] * mine + jnp.where(first_lane, l_in * theirs, 0.0)
        m_v[b] = m_new
        o_ref[n, 0:block] = o_ref[n, 0:block] * wide(mine, lat // 128) + carry[c, 0:block] * wide(theirs, lat // 128)

    for g in range(groups):
        weights[g].wait()
        if g == 0:
            wuk_copy.wait()
        project(hid_ref[...], cos_ref[...], sin_ref[...], g, store_own)
    for n in range(lat // 128):
        qs_v[:, n * 128:(n + 1) * 128] = qs_f[n].astype(BF16)
    qs_v[:, lat:lat + rope] = qs_f[lat // 128][:, 0:rope].astype(BF16)
    kv_copy.wait()
    kv_send.wait()
    outs = [pltpu.make_async_copy(qs_v, qs_hbm.at[0], out_sem.at[0])]
    own_targets, d_targets = [(6, own_v, 0), (7, own_v, 1)], [(4, diag, 0), (5, diag, 1)]
    plain, added = [(0, x_v, 0), (3, y_v, 1)], [(1, x_v, 1), (2, y_v, 0)]
    attend(own_targets[:1], between=outs)

    for copy in gathers:
        copy.wait()
    hid3 = hid_all[...].reshape(3 * rows, hid_ref.shape[1])
    cos3 = jnp.concatenate([cos_all[p] for p in range(3)], axis=0)
    sin3 = jnp.concatenate([sin_all[p] for p in range(3)], axis=0)
    for g in range(groups):
        project(hid3, cos3, sin3, g, store_peer)

    attend(d_targets)
    close(d_targets)
    over = [remote(diag.at[0], carry.at[0], 10, to_x), remote(diag.at[1], carry.at[1], 11, to_y)]
    attend(own_targets[1:], between=over)
    close(own_targets)
    outs.append(pltpu.make_async_copy(own_v, own_hbm, out_sem.at[5]))
    attend(plain, between=outs[1:])
    close(plain)
    early = [remote(x_v.at[0, 0:soon], soon_x_hbm, 12, to_x), remote(y_v.at[1, 0:soon], soon_y_hbm, 13, to_y)]
    outs.append(pltpu.make_async_copy(x_v.at[0, soon:block + TAIL], x_hbm.at[0:rest], out_sem.at[1]))
    outs.append(pltpu.make_async_copy(y_v.at[1, soon:block + TAIL], y_hbm.at[block + TAIL:rest + block + TAIL], out_sem.at[2]))
    attend(added, between=[*early, *outs[2:]])
    for copy in over:
        copy.wait()
    merge(1, x_v, 1, 1)
    merge(2, y_v, 0, 0)
    close(added)
    last = [pltpu.make_async_copy(x_v.at[1], x_hbm.at[rest:rest + block + TAIL], out_sem.at[3]),
            pltpu.make_async_copy(y_v.at[0], y_hbm.at[0:block + TAIL], out_sem.at[4])]
    for copy in last:
        copy.start()
    for copy in (*outs, *early, *last):
        copy.wait()


def prefix_phase(hidden, w_q, w_uk, kv_own, seq_lens, first_pos, log2_scale, chunk=1024, soon=96):
    rows, dim = hidden.shape
    n_head, nope, lat = w_uk.shape
    qk = w_q.shape[1] // n_head
    rope = qk - nope
    inv_freq = jnp.exp(jnp.arange(rope // 2, dtype=F32) * (-math.log(ROPE_BASE) / (rope // 2)))[None, :]
    block = n_head // 2 * rows
    payload = jax.ShapeDtypeStruct((2, block + TAIL, lat), F32)
    early = jax.ShapeDtypeStruct((soon, lat), F32)
    later = jax.ShapeDtypeStruct((2 * (block + TAIL) - soon, lat), F32)
    in_hbm = pl.BlockSpec(memory_space=pltpu.HBM)
    return pl.pallas_call(
        functools.partial(prefix_kernel, n_head, nope, rope, log2_scale, first_pos),
        out_shape=(jax.ShapeDtypeStruct((64, rows * n_head, lat + rope), BF16), payload, later, later, early, early),
        in_specs=[pl.BlockSpec(memory_space=pltpu.SMEM), in_hbm, vmem(), in_hbm, in_hbm, in_hbm],
        out_specs=(in_hbm,) * 6,
        scratch_shapes=[
            pltpu.VMEM((rows, dim), BF16), pltpu.VMEM((rows, rope // 2), F32), pltpu.VMEM((rows, rope // 2), F32),
            pltpu.VMEM((3, rows, dim), BF16), pltpu.VMEM((3, rows, rope // 2), F32), pltpu.VMEM((3, rows, rope // 2), F32),
            pltpu.VMEM(w_q.shape, BF16), pltpu.VMEM(w_uk.shape, BF16), pltpu.VMEM((2, *kv_own.shape), BF16),
            pltpu.VMEM((8, block, lat + rope), BF16), pltpu.VMEM((lat // 128 + 1, rows * n_head, 128), F32),
            pltpu.VMEM((rows * n_head, lat + rope), BF16),
            pltpu.VMEM((8, block, 128), F32), pltpu.VMEM((8, block, 128), F32),
            pltpu.VMEM((4, block, chunk), F32), pltpu.VMEM((4, block, chunk), BF16),
            *[pltpu.VMEM(payload.shape, F32)] * 5,
            pltpu.SemaphoreType.DMA((n_head // 4,)), pltpu.SemaphoreType.DMA((3,)), pltpu.SemaphoreType.DMA((6,)),
            pltpu.SemaphoreType.DMA((14,)), pltpu.SemaphoreType.DMA((14,))],
        compiler_params=pltpu.CompilerParams(collective_id=0, has_side_effects=True, vmem_limit_bytes=60 * MIB),
        name='prefix',
    )(seq_lens, hidden, inv_freq, w_q, w_uk, kv_own)


def suffix_kernel(log2_scale, lat, chunk, unit, ring, streamed, lens_ref, q_hbm, kv_hbm, o_ref, m_ref, l_ref,
                  q_ref, kv_v, s_v, m_v, l_v, acc, sems, q_sem, b_s, c_s):
    n_seq = lens_ref.shape[0]
    heads = q_hbm.shape[1] // n_seq
    shift = chunk.bit_length() - 1
    q_copy = pltpu.make_async_copy(q_hbm.at[0], q_ref, q_sem)
    q_copy.start()
    total = jnp.int32(0)
    for b in range(n_seq):
        total += lax.shift_right_logical(lens_ref[b], shift) + 1
    trips = lax.div(total + unit - 1, unit)
    depth = ring - 2

    def start(at, group, live):
        b, c = at
        for u in range(unit):
            b_s[group * unit + u] = b
            c_s[group * unit + u] = c
            have = jnp.minimum(b, n_seq - 1)

            @pl.when(live)
            def _(u=u, c=c, have=have):
                pltpu.make_async_copy(
                    kv_hbm.at[have, :, pl.ds(pl.multiple_of(c * chunk, chunk), chunk)], kv_v.at[group, u], sems.at[group]).start()
            last = c >= lax.shift_right_logical(lens_ref[have], shift)
            b, c = jnp.where(last, jnp.minimum(b + 1, n_seq), b), jnp.where(last, 0, c + 1)
        return b, c

    for u in range(unit):
        b_s[(ring - 1) * unit + u] = n_seq
        c_s[(ring - 1) * unit + u] = 0
    ahead = lax.fori_loop(0, depth, lambda j, at: start(at, j, j < trips), (jnp.int32(0), jnp.int32(0)))

    def step(i, at):
        base, prev, far = [lax.rem(i + d, ring) for d in (0, ring - 1, depth)]

        @pl.when(i < trips)
        def _():
            pltpu.make_async_copy(kv_v.at[base], kv_v.at[base], sems.at[base]).wait()

        here, there = lax.rem(i, 2), lax.rem(i + 1, 2)
        for u in range(unit):
            bq = jnp.minimum(b_s[base * unit + u], n_seq - 1)
            q = q_ref[pl.ds(pl.multiple_of(bq * heads, heads), heads), :]
            s_v[here, u] = jnp.dot(q, kv_v[base, u], preferred_element_type=F32)

        lanes = lax.broadcasted_iota(jnp.int32, (heads, chunk), 1)
        items = [(b_s[prev * unit + u], c_s[prev * unit + u]) for u in range(unit)]
        scores = []
        for u, (b, c) in enumerate(items):
            length = lens_ref[jnp.minimum(b, n_seq - 1)]
            scores.append(jnp.where(lanes <= length - c * chunk, s_v[there, u], -jnp.inf))
        top = jnp.max(jnp.concatenate(scores, axis=0), axis=1, keepdims=True)
        m_old, l_old, o_old = m_v[...], l_v[...], acc[...]
        for u, (b, c) in enumerate(items):
            first = c == 0
            m_old = jnp.where(first, -jnp.inf, m_old)
            m_new = jnp.maximum(m_old, top[u * heads:(u + 1) * heads])
            alpha = jnp.exp2((m_old - m_new) * log2_scale)
            p = jnp.exp2((scores[u] - wide(m_new, chunk // 128)) * log2_scale)
            part = p[:, 0:128]
            for n in range(1, chunk // 128):
                part += p[:, n * 128:(n + 1) * 128]
            if u in streamed:
                added = jnp.transpose(lax.dot_general(kv_v[prev, u, 0:lat, :], p.astype(BF16), NT, preferred_element_type=F32))
            else:
                added = lax.dot_general(p.astype(BF16), kv_v[prev, u, 0:lat, :], NT, preferred_element_type=F32)
            l_old = jnp.where(first, 0.0, l_old * alpha) + part
            o_old = jnp.where(first, 0.0, o_old * wide(alpha, lat // 128)) + added
            m_old = m_new
            out = pl.ds(pl.multiple_of(b * heads, heads), heads)
            m_ref[out, :] = m_old
            l_ref[out, :] = l_old
            for n in range(lat // 128):
                o_ref[n, out, :] = o_old[:, n * 128:(n + 1) * 128]
        m_v[...], l_v[...], acc[...] = m_old, l_old, o_old
        return start(at, far, i + depth < trips)

    q_copy.wait()
    lax.fori_loop(0, trips + 1, step, ahead)


def suffix_part(q_seq, kv_suffix, seq_lens, log2_scale, lat, chunk=256, unit=9, ring=5, streamed=(1, 3, 5)):
    n_seq, slots, wide_row = kv_suffix.shape
    rows = q_seq.shape[1]
    heads = rows // n_seq
    flops = 2 * rows * slots * (wide_row + lat) * 4
    return pl.pallas_call(
        functools.partial(suffix_kernel, log2_scale, lat, chunk, unit, ring, streamed),
        out_shape=(jax.ShapeDtypeStruct((lat // 128, rows + heads, 128), F32), jax.ShapeDtypeStruct((rows + heads, 128), F32),
                   jax.ShapeDtypeStruct((rows + heads, 128), F32)),
        in_specs=[pl.BlockSpec(memory_space=pltpu.SMEM), hbm(), hbm()],
        out_specs=(vmem(), vmem(), vmem()),
        scratch_shapes=[pltpu.VMEM(q_seq.shape[1:], BF16), pltpu.VMEM((ring, unit, wide_row, chunk), BF16), pltpu.VMEM((2, unit, heads, chunk), F32),
                        pltpu.VMEM((heads, 128), F32), pltpu.VMEM((heads, 128), F32),
                        pltpu.VMEM((heads, lat), F32), pltpu.SemaphoreType.DMA((ring,)), pltpu.SemaphoreType.DMA,
                        pltpu.SMEM((ring * unit,), jnp.int32), pltpu.SMEM((ring * unit,), jnp.int32)],
        compiler_params=pltpu.CompilerParams(vmem_limit_bytes=32 * MIB),
        cost_estimate=pl.CostEstimate(flops=flops, bytes_accessed=40 * MIB, transcendentals=0),
        name='suffix',
    )(seq_lens, q_seq, kv_suffix.swapaxes(1, 2))


def output_kernel(log2_scale, hid_ref, wuv_ref, wo_ref, so_ref, sm_ref, sl_ref, own_ref, x_ref, y_ref, soon_x_ref, soon_y_ref, out_ref):
    n_head = wuv_ref.shape[0]
    rows = hid_ref.shape[0]
    half = n_head // 2
    block = half * rows
    value = wuv_ref.shape[2]
    soon = soon_x_ref.shape[0]
    rest = block + TAIL - soon

    def sums_of(side, at):
        early = at < soon
        from_x = x_ref[rest + at:rest + at + rows] if side else soon_x_ref[at:at + rows] if early else x_ref[at - soon:at - soon + rows]
        low = block + TAIL + at - soon
        from_y = y_ref[at:at + rows] if not side else soon_y_ref[at:at + rows] if early else y_ref[low:low + rows]
        return own_ref[side, at:at + rows], from_x, from_y

    cols = []
    for side in range(2):
        x_low = rest + block if side else block - soon
        y_low = block + TAIL + block - soon if side else block
        for tail in (own_ref[side, block:block + TAIL], x_ref[x_low:x_low + TAIL], y_ref[y_low:y_low + TAIL]):
            cols.append((jnp.transpose(tail[:, 0:block])[:, 0:1], jnp.transpose(tail[:, block:2 * block])[:, 0:1]))
    out = hid_ref[...].astype(F32)
    values = []
    for h in range(n_head):
        side, at = h // half, (h % half) * rows
        mine = pl.ds(h, rows, stride=n_head)
        own = jnp.concatenate([so_ref[n, mine, :] for n in range(so_ref.shape[0])], axis=1)
        terms = [(own, sm_ref[mine, :][:, 0:1], jnp.sum(sl_ref[mine, :], axis=1, keepdims=True))]
        for k, o_part in enumerate(sums_of(side, at)):
            m_part, l_part = cols[side * 3 + k]
            terms.append((o_part, m_part[at:at + rows], l_part[at:at + rows]))
        m_all = functools.reduce(jnp.maximum, [t[1] for t in terms])
        o_sum, l_sum = 0.0, 0.0
        for o_part, m_part, l_part in terms:
            weight = jnp.exp2((m_part - m_all) * log2_scale)
            o_sum += o_part * weight
            l_sum += l_part * weight
        o_lat = (o_sum / l_sum).astype(BF16)
        values.append(jnp.dot(o_lat, wuv_ref[h], preferred_element_type=F32).astype(BF16))
        if len(values) == 4:
            low = (h - 3) * value
            out += jnp.dot(jnp.concatenate(values, axis=1), wo_ref[low:low + 4 * value], preferred_element_type=F32)
            values = []
    out_ref[...] = out.astype(BF16)


def finish_output(hidden, w_uv, w_o, suffix, parts, log2_scale):
    return pl.pallas_call(
        functools.partial(output_kernel, log2_scale),
        out_shape=jax.ShapeDtypeStruct(hidden.shape, BF16),
        in_specs=[vmem()] * 11,
        out_specs=vmem(),
        compiler_params=pltpu.CompilerParams(vmem_limit_bytes=32 * MIB),
        name='output',
    )(hidden, w_uv, w_o, *suffix, *parts)


def solution(mesh):
    group = mesh.shape['ctx']
    rows_spec = P(('dp', 'ctx'), None)
    whole_spec = P()
    over_x = [(i, i ^ 2) for i in range(group)]
    over_y = [(i, i ^ 4) for i in range(group)]

    def local_step(hidden, w_q, w_uk, w_uv, w_o, kv_prefix, kv_suffix, seq_lens):
        lat = w_uk.shape[2]
        n_head = w_uk.shape[0]
        log2_scale = LOG2E * (w_q.shape[1] // n_head) ** -0.5
        kv_own = kv_prefix.swapaxes(0, 1)
        q_seq, own, to_x, to_y, soon_x, soon_y = prefix_phase(hidden, w_q, w_uk, kv_own, seq_lens, kv_prefix.shape[0] * group, log2_scale)
        got_x, got_y = lax.ppermute(to_x, 'ctx', over_x), lax.ppermute(to_y, 'ctx', over_y)
        suffix = suffix_part(q_seq, kv_suffix, seq_lens, log2_scale, lat)
        return finish_output(hidden, w_uv, w_o, suffix, (own, got_x, got_y, soon_x, soon_y), log2_scale)

    return jax.shard_map(local_step, mesh=mesh, in_specs=(rows_spec, whole_spec, whole_spec, whole_spec, whole_spec, rows_spec, P(('dp', 'ctx'), None, None), P(('dp', 'ctx'))), out_specs=rows_spec, check_vma=False)
```
